128 devices in a mesh: shot: 4 (over y_hi, core), gx: 8 (over y_lo, z), gy: 4 (over x).
Axes of the slice: x: 4, y: 4 (y_hi: 2, y_lo: 2; y = y_hi * 2 + y_lo), z: 4, core: 2. Of those that a mesh axis runs over, the one named last changes fastest.
Arguments:
- state_now: float32 [4, 64, 256, 256], P('shot', 'gx', 'gy'), may hold values from -6 to 6
- state_prev: float32 [4, 64, 256, 256], P('shot', 'gx', 'gy'), may hold values from -6 to 6
- courant_sq: float32 [64, 256, 256], P('gx', 'gy'), may hold values from 0.03 to 0.3
- reflectivity: float32 [64, 256, 256], P('gx', 'gy'), may hold values from -6 to 6
- direction: float32 [64, 256, 256], P('gx', 'gy'), may hold values from -6 to 6
- prev_gradient: float32 [64, 256, 256], P('gx', 'gy'), may hold values from -3 to 3
- residual: float32 [4, 16, 64, 256], P('shot', None, 'gx', 'gy'), may hold values from -6 to 6
- rec_depth: int32 [4, 64, 256], P('shot', 'gx', 'gy'), may hold values from 0 to 255
- source_cell: int32 [4, 3], P('shot'), may hold values from 0 to 255, as said below
- wavelet: float32 [4, 15], P('shot'), may hold values from -80 to 80
- live_steps: int32 [4], P('shot'), may hold values from 8 to 16
Outputs:
- image_next: float32 [64, 256, 256], P('gx', 'gy')
- direction_next: float32 [64, 256, 256], P('gx', 'gy')
- residual_next: float32 [4, 16, 64, 256], P('shot', None, 'gx', 'gy')
- data_misfit: float32 [], replicated
The draws below stay inside these ranges and needn't reach their ends.
Inputs may be any that keep to these rules, and one draw needn't show every extreme that they name: `source_cell`: column 0 lies in 0 to 63, column 1 in 0 to 255, column 2 in 0 to 255.
All inputs are finite; a program needn't handle non-finite values.
Results may differ from the reference program's by a relative error of at most 0.0003.
Values sent between devices are 32-bit elements; how exact they have to be, the bound alone decides.
A program may use at most 64 MiB of HBM per device.

```python
import math
from functools import partial
import jax
import jax.numpy as jnp
from jax import lax

NT = 16
SHOTS = 4
NX = 64
NY = 256
NZ = 256


def draw_source_cell(key, part):
    keys = jax.random.split(jax.random.fold_in(key, 11), 3)
    first = jax.random.randint(keys[0], (SHOTS,), 0, NX)
    second = jax.random.randint(keys[1], (SHOTS,), 0, NY)
    third = jax.random.randint(keys[2], (SHOTS,), 0, NZ)
    return jnp.stack([first, second, third], axis=1).astype(jnp.int32)


def set_ends(array, key, least, top_value):
    dims = array.shape
    spot = [jax.random.randint(jax.random.fold_in(key, axis), (), 0, dims[axis]) for axis in range(len(dims))]
    array = array.at[tuple(spot)].set(least)
    longest = dims.index(max(dims))
    spot[longest] = (spot[longest] + 1) % dims[longest]
    return array.at[tuple(spot)].set(top_value)


def levels(own_key, extent, cuts, low, top_value):
    def one(dim, shards_of):
        heights = jax.random.uniform(jax.random.fold_in(jax.random.fold_in(own_key, 6), dim), (shards_of,), jnp.float32, low / len(cuts), top_value / len(cuts))
        return jnp.repeat(jnp.exp(heights), extent[dim] // shards_of).reshape((-1,) + (1,) * (len(extent) - dim - 1))

    level = one(*cuts[0])
    for cut in cuts[1:]:
        level = level * one(*cut)
    return level


def normal_values(key, dims, spread, bound, cuts=(), held_as=jnp.bfloat16):
    level = levels(key, dims, cuts, -0.22, 0.18) if cuts else 1.0
    values = jax.random.normal(key, dims, jnp.float32) * spread * level
    return jnp.minimum(jnp.maximum(values, -bound), bound).astype(held_as)


def setup_inputs(seed: int = 0) -> dict:
    streams_of = jax.random.split(jax.random.key(seed), 12)
    return {
        "state_now": normal_values(streams_of[0], (SHOTS, NX, NY, NZ), 1.0, 6.0, ((0, 4), (1, 8), (2, 4)), jnp.float32),
        "state_prev": normal_values(streams_of[1], (SHOTS, NX, NY, NZ), 1.0, 6.0, ((0, 4), (1, 8), (2, 4)), jnp.float32),
        "courant_sq": jnp.clip(jnp.exp(math.log(0.3) - 2.3025852 * jax.random.uniform(streams_of[2], (NX, NY, NZ), jnp.float32) ** levels(streams_of[2], (NX, NY, NZ), ((0, 8), (1, 4)), -0.2, 0.2)), 0.03, 0.3),
        "reflectivity": normal_values(streams_of[3], (NX, NY, NZ), 1.0, 6.0, ((0, 8), (1, 4)), jnp.float32),
        "direction": normal_values(streams_of[4], (NX, NY, NZ), 1.0, 6.0, ((0, 8), (1, 4)), jnp.float32),
        "prev_gradient": normal_values(streams_of[5], (NX, NY, NZ), 0.5, 3.0, ((0, 8), (1, 4)), jnp.float32),
        "residual": normal_values(streams_of[6], (SHOTS, NT, NX, NY), 1.0, 6.0, ((0, 4), (2, 8), (3, 4)), jnp.float32),
        "rec_depth": set_ends(jax.random.randint(streams_of[7], (SHOTS, NX, NY), 0, NZ), jax.random.fold_in(streams_of[7], 1), 0, NZ - 1).astype(jnp.int32),
        "source_cell": draw_source_cell(jax.random.fold_in(streams_of[11], 71), 0),
        "wavelet": normal_values(streams_of[9], (SHOTS, NT - 1), 20.0, 80.0, ((0, 4),), jnp.float32),
        "live_steps": set_ends(jax.random.randint(streams_of[10], (SHOTS,), NT // 2, NT + 1), jax.random.fold_in(streams_of[10], 1), NT // 2, NT).astype(jnp.int32),
    }


def laplace(values):
    padded = jnp.pad(values, 1)
    beside = padded[2:, 1:-1, 1:-1] + padded[:-2, 1:-1, 1:-1] + padded[1:-1, 2:, 1:-1] + padded[1:-1, :-2, 1:-1]
    beside = beside + padded[1:-1, 1:-1, 2:] + padded[1:-1, 1:-1, :-2]
    return beside - 6.0 * values


def background(courant_sq, start, before, amplitudes, cell):
    axis_x = jnp.arange(NX, dtype=jnp.int32)
    axis_y = jnp.arange(NY, dtype=jnp.int32)
    axis_z = jnp.arange(NZ, dtype=jnp.int32)
    spot = ((axis_x[:, None, None] == cell[0]) & (axis_y[None, :, None] == cell[1]) & (axis_z[None, None, :] == cell[2])).astype(jnp.float32)

    def advance(carry, amplitude):
        present, former = carry
        advanced = 2.0 * present - former + courant_sq * laplace(present) + amplitude * spot
        return (advanced, present), present

    (final_state, unused), history = lax.scan(advance, (start, before), amplitudes)
    return jnp.concatenate([history, final_state[None]], axis=0)


def receiver_mask(depth):
    axis_z = jnp.arange(NZ, dtype=jnp.int32)
    return (axis_z[None, None, :] == depth[:, :, None]).astype(jnp.float32)


def live_weights(count):
    return (jnp.arange(NT, dtype=jnp.int32) < count).astype(jnp.float32)


def shot_gradient(courant_sq, inputs):
    start, before, amplitudes, cell, depth, count, records = inputs
    stored = background(courant_sq, start, before, amplitudes, cell)
    mask = receiver_mask(depth)
    weighted = records * live_weights(count)[:, None, None]
    newest = mask * weighted[NT - 1][:, :, None]
    accumulated = stored[NT - 1] * newest

    def retreat(carry, pair):
        following, furthest, summed = carry
        weight, wavefield = pair
        scaled = courant_sq * following
        current = 2.0 * following - furthest + laplace(scaled) + mask * weight[:, :, None]
        return (current, following, summed + wavefield * current), None

    zeros = jnp.zeros_like(start)
    (unused_a, unused_b, accumulated), unused_c = lax.scan(retreat, (newest, zeros, accumulated), (weighted[:NT - 1], stored[:NT - 1]), reverse=True)
    return accumulated


def shot_records(courant_sq, gain, inputs):
    start, before, amplitudes, cell, depth, count = inputs
    stored = background(courant_sq, start, before, amplitudes, cell)
    mask = receiver_mask(depth)

    def advance(carry, wavefield):
        present, former = carry
        advanced = 2.0 * present - former + courant_sq * laplace(present) + gain * wavefield
        return (advanced, present), jnp.sum(mask * advanced, axis=2)

    zeros = jnp.zeros_like(start)
    unused, records = lax.scan(advance, (zeros, zeros), stored)
    return records * live_weights(count)[:, None, None]


def reference(state_now, state_prev, courant_sq, reflectivity, direction, prev_gradient, residual, rec_depth, source_cell, wavelet, live_steps):
    grads = lax.map(partial(shot_gradient, courant_sq), (state_now, state_prev, wavelet, source_cell, rec_depth, live_steps, residual))
    gradient = courant_sq * jnp.sum(grads, axis=0)
    grad_sq = jnp.sum(gradient * gradient)
    cross = jnp.sum(gradient * prev_gradient)
    old_sq = jnp.sum(prev_gradient * prev_gradient)
    beta_coef = (grad_sq - cross) / old_sq
    direction_next = gradient + beta_coef * direction
    slope = jnp.sum(gradient * direction_next)
    gain = courant_sq * direction_next
    records = lax.map(partial(shot_records, courant_sq, gain), (state_now, state_prev, wavelet, source_cell, rec_depth, live_steps))
    step_length = slope / jnp.sum(records * records)
    image_next = reflectivity + step_length * direction_next
    residual_next = residual - step_length * records
    data_misfit = 0.5 * jnp.mean(residual_next * residual_next)
    return image_next, direction_next, residual_next, data_misfit
```

```python
import functools

import jax
import jax.numpy as jnp
from jax import lax
from jax.experimental import pallas as pl
from jax.experimental.pallas import tpu as pltpu
from jax.sharding import PartitionSpec as P

MESH = pl.DeviceIdType.MESH
F32 = jnp.float32
WAYS = [(-1, 0), (1, 0), (0, -1), (0, 1), (-1, -1), (-1, 1), (1, -1), (1, 1)]
DEEP = 2
TILE = 8


def kernel(
    sizes,
    groups,
    now_h,
    prev_h,
    csq_h,
    refl_h,
    dirn_h,
    oldg_h,
    rec_h,
    source,
    wavelet,
    live,
    image_h,
    dirout_h,
    resid_h,
    misfit_o,
    back,
    adj,
    csq,
    dirn,
    grad,
    gain,
    spot,
    crec,
    recs,
    recv_mask,
    traces,
    oldg,
    refl,
    half_a,
    half_b,
    half_c,
    slots_a,
    slots_b,
    slots_c,
    local_sem,
    start_send,
    start_recv,
    halo_send,
    halo_recv,
    pair_send,
    pair_recv,
    sum_send,
    sum_recv,
    out_sem,
):
    nx, ny, nz, steps, entries = sizes
    shots, gxs, gys = groups
    ex, ey = nx + 2 * DEEP, ny + 2 * TILE
    x_lo, x_hi = DEEP, DEEP + nx
    y_lo, y_hi = TILE, TILE + ny
    shot, gx, gy = lax.axis_index("shot"), lax.axis_index("gx"), lax.axis_index("gy")
    core = lax.rem(shot, 2)

    def has(way):
        at_x, at_y = gx + way[0], gy + way[1]
        return (at_x >= 0) & (at_x < gxs) & (at_y >= 0) & (at_y < gys)

    def regions(way, width):
        dx, dy = way
        src_x, dst_x = {
            -1: ((x_lo, width), (x_hi, width)),
            1: ((x_hi - width, width), (x_lo - width, width)),
            0: ((x_lo, nx), (x_lo, nx)),
        }[dx]
        src_y, dst_y = {
            -1: ((y_lo, TILE), (y_hi, TILE)),
            1: ((y_hi - TILE, TILE), (0, TILE)),
            0: ((y_lo, ny), (y_lo, ny)),
        }[dy]
        return (
            (pl.ds(*src_x), pl.ds(*src_y), slice(None)),
            (pl.ds(*dst_x), pl.ds(*dst_y), slice(None)),
        )

    def halo_copy(ref, k, width, send, recv):
        src, dst = regions(WAYS[k], width)
        return pltpu.make_async_remote_copy(
            src_ref=ref.at[src],
            dst_ref=ref.at[dst],
            send_sem=send.at[k],
            recv_sem=recv.at[k],
            device_id={"gx": gx + WAYS[k][0], "gy": gy + WAYS[k][1]},
            device_id_type=MESH,
        )

    def start_way(ref, k, width, send, recv):
        @pl.when(has(WAYS[k]))
        def _():
            halo_copy(ref, k, width, send, recv).start()

    def start_halo(ref, width, send, recv):
        for k in range(8):
            start_way(ref, k, width, send, recv)

    def wait_halo(ref, width, send, recv):
        for k, way in enumerate(WAYS):
            came = has((-way[0], -way[1]))

            @pl.when(came)
            def _():
                halo_copy(ref, k, width, send, recv).wait_recv()

            @pl.when(jnp.logical_not(came))
            def _():
                where = regions(way, width)[1]
                view = ref.at[where]
                view[...] = jnp.zeros(view.shape, F32)

            @pl.when(has(way))
            def _():
                halo_copy(ref, k, width, send, recv).wait_send()

    inner = (pl.ds(x_lo, nx), pl.ds(y_lo, ny), slice(None))
    loads = [
        (rec_h, traces.at[inner]),
        (csq_h, csq.at[inner]),
        (now_h, back.at[(1,) + inner]),
        (prev_h, back.at[(0,) + inner]),
        (dirn_h, dirn.at[inner]),
        (oldg_h, oldg),
        (refl_h, refl),
    ]
    copies = [
        pltpu.make_async_copy(src, dst, local_sem.at[i]) for i, (src, dst) in enumerate(loads)
    ]
    for copy in copies:
        copy.start()
    starts = [(traces, DEEP), (csq, DEEP), (back.at[1], DEEP), (back.at[0], 1), (dirn, DEEP)]
    for i in range(4):
        copies[i].wait()
        start_halo(starts[i][0], starts[i][1], start_send.at[i], start_recv.at[i])
    for i in range(4, 7):
        copies[i].wait()

    lane = lax.broadcasted_iota(jnp.int32, (ey, nz), 1)
    lane_t = lax.broadcasted_iota(jnp.int32, (ey, 128), 1)
    row = lax.broadcasted_iota(jnp.int32, (ey, nz), 0)
    first, last = lane == 0, lane == nz - 1
    live_here = live[0]
    yz = (row + (gy * ny - TILE) == source[0, 1]) & (lane == source[0, 2])

    @pl.loop(0, ex)
    def _(i):
        adj[0, i] = jnp.zeros((ey, nz), F32)
        hit = yz & (row * 0 + (i + gx * nx - DEEP) == source[0, 0])
        spot[i] = jnp.where(hit, 1.0, 0.0)

    recs[...] = jnp.zeros(recs.shape, F32)
    wait_halo(traces, DEEP, start_send.at[0], start_recv.at[0])
    wait_halo(csq, DEEP, start_send.at[1], start_recv.at[1])

    def column(i, n):
        picked = jnp.where((lane_t == n) & (lane_t < live_here), traces[i], 0.0)
        return jnp.sum(picked, axis=1, keepdims=True)

    @pl.loop(0, ex)
    def _(i):
        depth = jnp.sum(jnp.where(lane_t == steps, traces[i], 0.0), axis=1, keepdims=True)
        here = lane.astype(F32) == depth
        crec[i] = jnp.where(here, csq[i], 0.0)
        adj[1, i] = crec[i] * column(i, steps - 1)

    @pl.loop(0, nx)
    def _(i):
        depth = jnp.sum(
            jnp.where(lane_t == steps, traces[i + x_lo], 0.0), axis=1, keepdims=True
        )
        here = lane.astype(F32) == depth
        recv_mask[i] = jnp.where(here, 1.0, 0.0)[y_lo:y_hi]

    def plane(field, s, i, whole, extra):
        v = field[s, i]
        cut = slice(0, ey) if whole else slice(y_lo, y_hi)
        rows = pl.ds(0, ey) if whole else pl.ds(y_lo, ny)
        mid = v[cut]
        total = field[s, i - 1, rows, :] + field[s, i + 1, rows, :]
        total = total + (pltpu.roll(v, 1, 0) + pltpu.roll(v, ey - 1, 0))[cut]
        left = jnp.where(first[cut], 0.0, pltpu.roll(mid, 1, 1))
        right = jnp.where(last[cut], 0.0, pltpu.roll(mid, nz - 1, 1))
        total = total + left + right
        value = csq[i, rows, :] * (total - 6.0 * mid)
        value = value + (2.0 * mid - field[s - 1, i, rows, :]) + extra(i, rows, cut)
        field[s + 1, i, rows, :] = value

    def planes(field, s, lo, hi, whole, extra):
        @pl.loop(lo, hi)
        def _(i):
            plane(field, s, i, whole, extra)

    def ahead(s):
        amount = wavelet[0, s - 1]
        return lambda i, rows, cut: amount * spot[i, rows, :]

    def behind(s):
        return lambda i, rows, cut: crec[i, rows, :] * column(i, steps - 1 - s)[cut]

    def scattered(s):
        return lambda i, rows, cut: gain[i, rows, :] * back[s + 1, i, rows, :]

    def advance(field, s, make, send, recv):
        planes(field, s, x_lo - 1, x_hi + 1, True, make(s))
        extra = make(s + 1)
        target = field.at[s + 2]
        planes(field, s + 1, x_lo, x_lo + DEEP, False, extra)
        start_way(target, 0, DEEP, send, recv)
        planes(field, s + 1, x_hi - DEEP, x_hi, False, extra)
        start_way(target, 1, DEEP, send, recv)
        for k in range(4, 8):
            start_way(target, k, DEEP, send, recv)
        planes(field, s + 1, x_lo + DEEP, x_hi - DEEP, False, extra)
        start_way(target, 2, DEEP, send, recv)
        start_way(target, 3, DEEP, send, recv)

    blocks = (steps - 1) // 2

    @pl.loop(0, blocks)
    def _(j):
        s = 2 * j + 1
        now, before = lax.rem(j, 2), lax.rem(j + 1, 2)
        for field, way, make in ((adj, 1, behind), (back, 0, ahead)):

            @pl.when(j > 0)
            def _():
                wait_halo(field.at[s], DEEP, halo_send.at[way, before], halo_recv.at[way, before])

            if way == 0:

                @pl.when(j == 0)
                def _():
                    wait_halo(back.at[1], DEEP, start_send.at[2], start_recv.at[2])
                    wait_halo(back.at[0], 1, start_send.at[3], start_recv.at[3])

            advance(field, s, make, halo_send.at[way, now], halo_recv.at[way, now])

    end = 2 * blocks + 1
    final = (blocks - 1) % 2
    for field, way, make in ((adj, 1, behind), (back, 0, ahead)):
        wait_halo(field.at[end], DEEP, halo_send.at[way, final], halo_recv.at[way, final])
        planes(field, end, x_lo, x_hi, False, make(end))

    start_halo(dirn, DEEP, start_send.at[4], start_recv.at[4])

    half = nx // 2
    partner = {"shot": shot + 1 - 2 * core}
    opposite = {"shot": lax.rem(shot + 2, shots)}
    mine, other = x_lo + half * core, x_lo + half * (1 - core)
    own_half = (pl.ds(mine, half), pl.ds(y_lo, ny), slice(None))

    def products(start, keep):
        @pl.loop(start, start + half)
        def _(i):
            total = back[1, i, y_lo:y_hi, :] * adj[steps, i, y_lo:y_hi, :]
            for a in range(2, steps + 1):
                total = total + back[a, i, y_lo:y_hi, :] * adj[steps + 1 - a, i, y_lo:y_hi, :]
            keep(i, total)

    def pair_copy(src, dst, k, device):
        return pltpu.make_async_remote_copy(
            src_ref=src,
            dst_ref=dst,
            send_sem=pair_send.at[k],
            recv_sem=pair_recv.at[k],
            device_id=device,
            device_id_type=MESH,
        )

    def keep_other(i, total):
        half_c[i - other] = total

    def keep_mine(i, total):
        grad[i, y_lo:y_hi, :] = total

    products(other, keep_other)
    swap_a = pair_copy(half_c, half_a, 0, partner)
    swap_a.start()
    products(mine, keep_mine)
    swap_a.wait()

    def add_half(buffer):
        @pl.loop(0, half)
        def _(i):
            grad[mine + i, y_lo:y_hi, :] = grad[mine + i, y_lo:y_hi, :] + buffer[i]

    add_half(half_a)
    swap_b = pair_copy(grad.at[own_half], half_b, 1, opposite)
    swap_b.start()
    swap_b.wait()
    add_half(half_b)
    spread = pair_copy(grad.at[own_half], grad.at[own_half], 2, partner)
    spread.start()

    def fold(values):
        return jnp.sum(values.reshape(-1, 8, 128), axis=0)

    def lanes(values):
        return values[:, :128] + values[:, 128:]

    def dots(i, sums):
        g = grad[mine + i, y_lo:y_hi, :]
        o = oldg[mine + i - x_lo]
        d = dirn[mine + i, y_lo:y_hi, :]
        parts = [fold(lanes(a * b)) for a, b in ((g, g), (g, o), (o, o), (g, d))]
        return tuple(s + p for s, p in zip(sums, parts))

    zero = jnp.zeros((8, 128), F32)
    sums = lax.fori_loop(0, half, dots, (zero,) * 4)
    gy_core = gys * 2
    place = gy * 2 + core

    def gx_member(k):
        return {"gx": k}

    def side_member(k):
        return {"gy": k // 2, "shot": shot - core + lax.rem(k, 2)}

    def all_sum(values, slots, at, count, member, base):
        slots[at] = values

        def copy(peer, slot):
            return pltpu.make_async_remote_copy(
                src_ref=slots.at[at],
                dst_ref=slots.at[slot],
                send_sem=sum_send.at[base, peer],
                recv_sem=sum_recv.at[base, slot],
                device_id=member(peer),
                device_id_type=MESH,
            )

        for o in range(1, count):
            copy(lax.rem(at + o, count), at).start()
        for o in range(1, count):
            source_at = lax.rem(at + count - o, count)
            copy(source_at, source_at).wait_recv()
        for o in range(1, count):
            copy(lax.rem(at + o, count), at).wait_send()
        total = slots[0]
        for k in range(1, count):
            total = total + slots[k]
        return total

    def reduce_all(values):
        return jnp.sum(jnp.sum(values, axis=1, keepdims=True), axis=0, keepdims=True)

    stacked = jnp.stack(sums)
    spread.wait_recv()
    start_halo(grad, DEEP, start_send.at[0], start_recv.at[0])
    stacked = all_sum(stacked, slots_a.at[0], gx, gxs, gx_member, 0)
    stacked = all_sum(stacked, slots_b.at[0], place, gy_core, side_member, 1)
    grad_sq, cross, old_sq, toward = [reduce_all(stacked[k]) for k in range(4)]
    beta = (grad_sq - cross) / old_sq
    slope = grad_sq + beta * toward
    spread.wait_send()
    wait_halo(dirn, DEEP, start_send.at[4], start_recv.at[4])
    wait_halo(grad, DEEP, start_send.at[0], start_recv.at[0])

    @pl.loop(0, ex)
    def _(i):
        onward = grad[i] + beta * dirn[i]
        dirn[i] = onward
        gain[i] = csq[i] * onward
        adj[1, i] = gain[i] * back[1, i]

    def sample(s):
        @pl.loop(0, nx)
        def _(i):
            seen = adj[s, i + x_lo, y_lo:y_hi, :] * recv_mask[i]
            value = jnp.sum(seen, axis=1, keepdims=True)
            recs[i] = jnp.where(lane_t[:ny] == s - 1, value, recs[i])

    out_dir = pltpu.make_async_copy(dirn.at[inner], dirout_h, out_sem.at[0])
    sample(1)
    out_dir.start()

    @pl.loop(0, blocks)
    def _(j):
        s = 2 * j + 1
        now, before = lax.rem(j, 2), lax.rem(j + 1, 2)

        @pl.when(j > 0)
        def _():
            wait_halo(adj.at[s], DEEP, halo_send.at[2, before], halo_recv.at[2, before])

        advance(adj, s, scattered, halo_send.at[2, now], halo_recv.at[2, now])
        sample(s + 1)
        sample(s + 2)

    wait_halo(adj.at[end], DEEP, halo_send.at[2, final], halo_recv.at[2, final])
    planes(adj, end, x_lo, x_hi, False, scattered(end))
    sample(end + 1)

    lane_r = lane_t[:ny]
    told = lane_r < live_here
    kept = lane_r < steps

    def score(i, sums):
        rec = jnp.where(told, recs[i], 0.0)
        res = jnp.where(kept, traces[i + x_lo, y_lo:y_hi, :], 0.0)
        recs[i] = rec
        parts = [fold(a * b) for a, b in ((rec, rec), (rec, res), (res, res))]
        return tuple(s + p for s, p in zip(sums, parts))

    sums = lax.fori_loop(0, nx, score, (zero,) * 3)
    stacked = jnp.stack(sums + (zero,))
    stacked = all_sum(stacked, slots_a.at[1], gx, gxs, gx_member, 2)
    stacked = all_sum(stacked, slots_b.at[1], place, gy_core, side_member, 3)
    upper = shot // 2
    stacked = all_sum(
        stacked, slots_c, upper, shots // 2, lambda k: {"shot": k * 2 + core}, 4
    )
    rec_sq, rec_res, res_sq = [reduce_all(stacked[k]) for k in range(3)]
    length = slope / rec_sq

    @pl.loop(0, nx)
    def _(i):
        refl[i] = refl[i] + length * dirn[i + x_lo, y_lo:y_hi, :]

    out_image = pltpu.make_async_copy(refl, image_h, out_sem.at[1])
    out_image.start()

    @pl.loop(0, nx)
    def _(i):
        recs[i] = traces[i + x_lo, y_lo:y_hi, :] - length * recs[i]

    out_resid = pltpu.make_async_copy(recs, resid_h, out_sem.at[2])
    out_resid.start()
    misfit = res_sq - 2.0 * length * rec_res + length * length * rec_sq
    misfit_o[...] = jnp.broadcast_to(misfit * (0.5 / entries), (8, 128))
    out_dir.wait()
    out_image.wait()
    out_resid.wait()


def on_device(groups, *arguments):
    (now, prev, csq, refl, dirn, oldg, residual, depth, source, wavelet, live) = arguments
    now, prev = now[0], prev[0]
    nx, ny, nz = now.shape
    steps = residual.shape[1]
    entries = float(residual.size * groups[0] * groups[1] * groups[2])
    ex, ey = nx + 2 * DEEP, ny + 2 * TILE
    traces = jnp.concatenate([residual[0], depth.astype(F32)], axis=0)
    traces = jnp.pad(jnp.transpose(traces, (1, 2, 0)), ((0, 0), (0, 0), (0, 127 - steps)))
    whole = pl.BlockSpec(memory_space=pl.ANY)
    small = pl.BlockSpec(memory_space=pltpu.SMEM)
    grow = pltpu.VMEM((ex, ey, nz), F32)
    dma = pltpu.SemaphoreType.DMA
    image, onward, resid, misfit = pl.pallas_call(
        functools.partial(kernel, (nx, ny, nz, steps, entries), groups),
        out_shape=(
            jax.ShapeDtypeStruct((nx, ny, nz), F32),
            jax.ShapeDtypeStruct((nx, ny, nz), F32),
            jax.ShapeDtypeStruct((nx, ny, 128), F32),
            jax.ShapeDtypeStruct((8, 128), F32),
        ),
        in_specs=[whole] * 7 + [small] * 3,
        out_specs=(whole, whole, whole, pl.BlockSpec(memory_space=pltpu.VMEM)),
        scratch_shapes=[
            pltpu.VMEM((steps + 1, ex, ey, nz), F32),
            pltpu.VMEM((steps + 1, ex, ey, nz), F32),
            grow,
            grow,
            grow,
            grow,
            grow,
            grow,
            pltpu.VMEM((nx, ny, 128), F32),
            pltpu.VMEM((nx, ny, nz), F32),
            pltpu.VMEM((ex, ey, 128), F32),
            pltpu.VMEM((nx, ny, nz), F32),
            pltpu.VMEM((nx, ny, nz), F32),
            pltpu.VMEM((nx // 2, ny, nz), F32),
            pltpu.VMEM((nx // 2, ny, nz), F32),
            pltpu.VMEM((nx // 2, ny, nz), F32),
            pltpu.VMEM((2, groups[1], 4, 8, 128), F32),
            pltpu.VMEM((2, groups[2] * 2, 4, 8, 128), F32),
            pltpu.VMEM((groups[0] // 2, 4, 8, 128), F32),
            dma((7,)),
            dma((5, 8)),
            dma((5, 8)),
            dma((3, 2, 8)),
            dma((3, 2, 8)),
            dma((3,)),
            dma((3,)),
            dma((5, 8)),
            dma((5, 8)),
            dma((3,)),
        ],
        compiler_params=pltpu.CompilerParams(
            has_side_effects=True, vmem_limit_bytes=62 * 1024 * 1024
        ),
        name="iteration",
    )(now, prev, csq, refl, dirn, oldg, traces, source, wavelet, live)
    resid = jnp.transpose(resid[:, :, :steps], (2, 0, 1))[None]
    return image, onward, resid, misfit[0, 0]


def solution(mesh):
    groups = (mesh.shape["shot"], mesh.shape["gx"], mesh.shape["gy"])
    space = P("gx", "gy", None)
    placed = (
        P("shot", "gx", "gy", None),
        P("shot", "gx", "gy", None),
        space,
        space,
        space,
        space,
        P("shot", None, "gx", "gy"),
        P("shot", "gx", "gy"),
        P("shot", None),
        P("shot", None),
        P("shot"),
    )
    return jax.shard_map(
        functools.partial(on_device, groups),
        mesh=mesh,
        in_specs=placed,
        out_specs=(space, space, P("shot", None, "gx", "gy"), P()),
        check_vma=False,
    )
```

```python
import functools

import jax
import jax.numpy as jnp
from jax import lax
from jax.experimental import pallas as pl
from jax.experimental.pallas import tpu as pltpu
from jax.sharding import PartitionSpec as P

MESH = pl.DeviceIdType.MESH
F32 = jnp.float32
WAYS = [(-1, 0), (1, 0), (0, -1), (0, 1), (-1, -1), (-1, 1), (1, -1), (1, 1)]
DEEP = 2
TILE = 8
LANES = 128


def kernel(
    sizes,
    groups,
    now_h,
    prev_h,
    csq_h,
    refl_h,
    dirn_h,
    oldg_h,
    rec_h,
    source,
    wavelet,
    live,
    image_h,
    dirout_h,
    resid_h,
    misfit_o,
    back,
    adj,
    csq,
    dirn,
    grad,
    gain,
    spot,
    crec,
    twice,
    recs,
    recv_mask,
    traces,
    oldg,
    refl,
    half_a,
    half_b,
    half_c,
    slots_a,
    slots_b,
    slots_c,
    local_sem,
    start_send,
    start_recv,
    halo_send,
    halo_recv,
    pair_send,
    pair_recv,
    sum_send,
    sum_recv,
    out_sem,
):
    nx, ny, nz, steps, entries = sizes
    shots, gxs, gys = groups
    parts = nz // LANES
    ex, ey = nx + 2 * DEEP, ny + 2 * TILE
    x_lo, x_hi = DEEP, DEEP + nx
    y_lo, y_hi = TILE, TILE + ny
    shot, gx, gy = lax.axis_index("shot"), lax.axis_index("gx"), lax.axis_index("gy")
    core = lax.rem(shot, 2)

    def has(way):
        at_x, at_y = gx + way[0], gy + way[1]
        return (at_x >= 0) & (at_x < gxs) & (at_y >= 0) & (at_y < gys)

    def regions(way, width):
        dx, dy = way
        src_x, dst_x = {
            -1: ((x_lo, width), (x_hi, width)),
            1: ((x_hi - width, width), (x_lo - width, width)),
            0: ((x_lo, nx), (x_lo, nx)),
        }[dx]
        src_y, dst_y = {
            -1: ((y_lo, TILE), (y_hi, TILE)),
            1: ((y_hi - TILE, TILE), (0, TILE)),
            0: ((y_lo, ny), (y_lo, ny)),
        }[dy]
        return (
            (pl.ds(*src_x), slice(None), pl.ds(*src_y), slice(None)),
            (pl.ds(*dst_x), slice(None), pl.ds(*dst_y), slice(None)),
        )

    def halo_copy(ref, k, width, send, recv):
        src, dst = regions(WAYS[k], width)
        return pltpu.make_async_remote_copy(
            src_ref=ref.at[src],
            dst_ref=ref.at[dst],
            send_sem=send.at[k],
            recv_sem=recv.at[k],
            device_id={"gx": gx + WAYS[k][0], "gy": gy + WAYS[k][1]},
            device_id_type=MESH,
        )

    def start_way(ref, k, width, send, recv):
        @pl.when(has(WAYS[k]))
        def _():
            halo_copy(ref, k, width, send, recv).start()

    def start_halo(ref, width, send, recv):
        for k in range(8):
            start_way(ref, k, width, send, recv)

    def wait_halo(ref, width, send, recv):
        for k, way in enumerate(WAYS):
            came = has((-way[0], -way[1]))

            @pl.when(came)
            def _():
                halo_copy(ref, k, width, send, recv).wait_recv()

            @pl.when(jnp.logical_not(came))
            def _():
                where = regions(way, width)[1]
                view = ref.at[where]
                view[...] = jnp.zeros(view.shape, F32)

            @pl.when(has(way))
            def _():
                halo_copy(ref, k, width, send, recv).wait_send()

    xs, ys = pl.ds(x_lo, nx), pl.ds(y_lo, ny)

    def halves(array, view):
        return [
            (array.at[:, :, pl.ds(h * LANES, LANES)], view.at[:, h]) for h in range(parts)
        ]

    def inside(ref):
        return ref.at[xs, :, ys, :]

    loads = [
        [(rec_h, traces.at[xs, 0, ys, :])],
        halves(csq_h, inside(csq)),
        halves(now_h, inside(back.at[1])),
        halves(prev_h, inside(back.at[0])),
        halves(dirn_h, inside(dirn)),
        halves(oldg_h, oldg),
        halves(refl_h, refl),
    ]
    copies = [
        [pltpu.make_async_copy(src, dst, local_sem.at[i, h]) for h, (src, dst) in enumerate(pairs)]
        for i, pairs in enumerate(loads)
    ]
    for pairs in copies:
        for copy in pairs:
            copy.start()
    starts = [(traces, DEEP), (csq, DEEP), (back.at[1], DEEP), (back.at[0], 1), (dirn, DEEP)]
    for i in range(4):
        for copy in copies[i]:
            copy.wait()
        start_halo(starts[i][0], starts[i][1], start_send.at[i], start_recv.at[i])
    for i in range(4, 7):
        for copy in copies[i]:
            copy.wait()

    lane = lax.broadcasted_iota(jnp.int32, (ey, LANES), 1)
    row = lax.broadcasted_iota(jnp.int32, (ey, LANES), 0)
    live_here = live[0]

    @pl.loop(0, ex)
    def _(i):
        for h in range(parts):
            adj[0, i, h] = jnp.zeros((ey, LANES), F32)
            hit = (row + (gy * ny - TILE) == source[0, 1]) & (lane + h * LANES == source[0, 2])
            hit = hit & (row * 0 + (i + gx * nx - DEEP) == source[0, 0])
            spot[i, h] = jnp.where(hit, 1.0, 0.0)

    recs[...] = jnp.zeros(recs.shape, F32)
    wait_halo(traces, DEEP, start_send.at[0], start_recv.at[0])
    wait_halo(csq, DEEP, start_send.at[1], start_recv.at[1])

    def column(i, n, r, count):
        at = lane[:count]
        picked = jnp.where((at == n) & (at < live_here), traces[i, 0, r : r + count, :], 0.0)
        return jnp.sum(picked, axis=1, keepdims=True)

    def receivers(i):
        level = jnp.sum(jnp.where(lane == steps, traces[i, 0], 0.0), axis=1, keepdims=True)
        return [(lane + h * LANES).astype(F32) == level for h in range(parts)]

    @pl.loop(0, ex)
    def _(i):
        newest = column(i, steps - 1, 0, ey)
        for h, here in enumerate(receivers(i)):
            crec[i, h] = jnp.where(here, csq[i, h], 0.0)
            adj[1, i, h] = crec[i, h] * newest
            twice[i, h] = 2.0 - 6.0 * csq[i, h]

    @pl.loop(0, nx)
    def _(i):
        for h, here in enumerate(receivers(i + x_lo)):
            recv_mask[i, h] = jnp.where(here, 1.0, 0.0)[y_lo:y_hi]

    def strip(field, s, i, r, count, extra):
        at = lane[:count]
        first, last = at == 0, at == LANES - 1
        rows = pl.ds(r, count)
        mids = [field[s, i, h, rows, :] for h in range(parts)]
        ups = [pltpu.roll(mid, 1, 1) for mid in mids]
        downs = [pltpu.roll(mid, LANES - 1, 1) for mid in mids]
        for h, mid in enumerate(mids):
            before = ups[h - 1] if h > 0 else 0.0
            after = downs[h + 1] if h < parts - 1 else 0.0
            left = jnp.where(first, before, ups[h])
            right = jnp.where(last, after, downs[h])
            if r > 0:
                above = field[s, i, h, pl.ds(r - 1, count), :]
            else:
                above = pltpu.roll(mid, 1, 0)
            if r + count < ey:
                below = field[s, i, h, pl.ds(r + 1, count), :]
            else:
                below = pltpu.roll(mid, count - 1, 0)
            total = (field[s, i - 1, h, rows, :] + field[s, i + 1, h, rows, :]) + (above + below)
            total = total + (left + right)
            value = csq[i, h, rows, :] * total + twice[i, h, rows, :] * mid
            value = value - field[s - 1, i, h, rows, :] + extra(i, h, r, count)
            field[s + 1, i, h, rows, :] = value

    def plane(field, s, i, whole, extra):
        if whole:
            strip(field, s, i, 0, TILE, extra(i, 0, TILE))
        strip(field, s, i, y_lo, ny, extra(i, y_lo, ny))
        if whole:
            strip(field, s, i, y_hi, TILE, extra(i, y_hi, TILE))

    def planes(field, s, lo, hi, whole, extra):
        @pl.loop(lo, hi, unroll=2)
        def _(i):
            plane(field, s, i, whole, extra)

    def ahead(s):
        amount = wavelet[0, s - 1]
        return lambda *_: lambda i, h, r, count: amount * spot[i, h, r : r + count, :]

    def behind(s):
        def at_plane(i, r, count):
            weight = column(i, steps - 1 - s, r, count)
            return lambda i, h, r, count: crec[i, h, r : r + count, :] * weight

        return at_plane

    def scattered(s):
        return lambda *_: (
            lambda i, h, r, count: gain[i, h, r : r + count, :] * back[s + 1, i, h, r : r + count, :]
        )

    def advance(field, s, make, send, recv):
        planes(field, s, x_lo - 1, x_hi + 1, True, make(s))
        extra = make(s + 1)
        target = field.at[s + 2]
        planes(field, s + 1, x_lo, x_lo + DEEP, False, extra)
        start_way(target, 0, DEEP, send, recv)
        planes(field, s + 1, x_hi - DEEP, x_hi, False, extra)
        start_way(target, 1, DEEP, send, recv)
        for k in range(4, 8):
            start_way(target, k, DEEP, send, recv)
        planes(field, s + 1, x_lo + DEEP, x_hi - DEEP, False, extra)
        start_way(target, 2, DEEP, send, recv)
        start_way(target, 3, DEEP, send, recv)

    blocks = (steps - 1) // 2

    @pl.loop(0, blocks)
    def _(j):
        s = 2 * j + 1
        now, before = lax.rem(j, 2), lax.rem(j + 1, 2)
        for field, way, make in ((adj, 1, behind), (back, 0, ahead)):

            @pl.when(j > 0)
            def _():
                wait_halo(field.at[s], DEEP, halo_send.at[way, before], halo_recv.at[way, before])

            if way == 0:

                @pl.when(j == 0)
                def _():
                    wait_halo(back.at[1], DEEP, start_send.at[2], start_recv.at[2])
                    wait_halo(back.at[0], 1, start_send.at[3], start_recv.at[3])

            advance(field, s, make, halo_send.at[way, now], halo_recv.at[way, now])

    end = 2 * blocks + 1
    final = (blocks - 1) % 2
    for field, way, make in ((adj, 1, behind), (back, 0, ahead)):
        wait_halo(field.at[end], DEEP, halo_send.at[way, final], halo_recv.at[way, final])
        planes(field, end, x_lo, x_hi, False, make(end))

    start_halo(dirn, DEEP, start_send.at[4], start_recv.at[4])

    half = nx // 2
    partner = {"shot": shot + 1 - 2 * core}
    opposite = {"shot": lax.rem(shot + 2, shots)}
    mine, other = x_lo + half * core, x_lo + half * (1 - core)
    own_half = (pl.ds(mine, half), slice(None), ys, slice(None))

    def products(start, keep):
        @pl.loop(start, start + half)
        def _(i):
            for h in range(parts):
                total = back[1, i, h, y_lo:y_hi, :] * adj[steps, i, h, y_lo:y_hi, :]
                for a in range(2, steps + 1):
                    one, two = back[a, i, h, y_lo:y_hi, :], adj[steps + 1 - a, i, h, y_lo:y_hi, :]
                    total = total + one * two
                keep(i, h, total)

    def pair_copy(src, dst, k, device):
        return pltpu.make_async_remote_copy(
            src_ref=src,
            dst_ref=dst,
            send_sem=pair_send.at[k],
            recv_sem=pair_recv.at[k],
            device_id=device,
            device_id_type=MESH,
        )

    def keep_other(i, h, total):
        half_c[i - other, h] = total

    def keep_mine(i, h, total):
        grad[i, h, y_lo:y_hi, :] = total

    products(other, keep_other)
    swap_a = pair_copy(half_c, half_a, 0, partner)
    swap_a.start()
    products(mine, keep_mine)
    swap_a.wait()

    def add_half(buffer):
        @pl.loop(0, half)
        def _(i):
            for h in range(parts):
                was = grad[mine + i, h, y_lo:y_hi, :]
                grad[mine + i, h, y_lo:y_hi, :] = was + buffer[i, h]

    add_half(half_a)
    swap_b = pair_copy(grad.at[own_half], half_b, 1, opposite)
    swap_b.start()
    swap_b.wait()
    add_half(half_b)
    spread = pair_copy(grad.at[own_half], grad.at[own_half], 2, partner)
    spread.start()

    def fold(values):
        return jnp.sum(values.reshape(-1, 8, LANES), axis=0)

    def dots(i, sums):
        for h in range(parts):
            g = grad[mine + i, h, y_lo:y_hi, :]
            o = oldg[mine + i - x_lo, h]
            d = dirn[mine + i, h, y_lo:y_hi, :]
            added = [fold(a * b) for a, b in ((g, g), (g, o), (o, o), (g, d))]
            sums = tuple(s + p for s, p in zip(sums, added))
        return sums

    zero = jnp.zeros((8, LANES), F32)
    eight = lax.broadcasted_iota(jnp.int32, (8, LANES), 0)

    def pack(sums):
        packed = zero
        for k, value in enumerate(sums):
            packed = jnp.where(eight == k, jnp.sum(value, axis=0, keepdims=True), packed)
        return packed

    def unpack(packed, k):
        return jnp.sum(packed[k : k + 1], axis=1, keepdims=True)

    sums = lax.fori_loop(0, half, dots, (zero,) * 4)
    gy_core = gys * 2
    place = gy * 2 + core

    def gx_member(k):
        return {"gx": k}

    def side_member(k):
        return {"gy": k // 2, "shot": shot - core + lax.rem(k, 2)}

    def all_sum(values, slots, at, count, member, base):
        slots[at] = values

        def copy(peer, slot):
            return pltpu.make_async_remote_copy(
                src_ref=slots.at[at],
                dst_ref=slots.at[slot],
                send_sem=sum_send.at[base, peer],
                recv_sem=sum_recv.at[base, slot],
                device_id=member(peer),
                device_id_type=MESH,
            )

        for o in range(1, count):
            copy(lax.rem(at + o, count), at).start()
        for o in range(1, count):
            source_at = lax.rem(at + count - o, count)
            copy(source_at, source_at).wait_recv()
        for o in range(1, count):
            copy(lax.rem(at + o, count), at).wait_send()
        total = slots[0]
        for k in range(1, count):
            total = total + slots[k]
        return total

    stacked = pack(sums)
    spread.wait_recv()
    start_halo(grad, DEEP, start_send.at[0], start_recv.at[0])
    stacked = all_sum(stacked, slots_a.at[0], gx, gxs, gx_member, 0)
    stacked = all_sum(stacked, slots_b.at[0], place, gy_core, side_member, 1)
    grad_sq, cross, old_sq, toward = [unpack(stacked, k) for k in range(4)]
    beta = (grad_sq - cross) / old_sq
    slope = grad_sq + beta * toward
    spread.wait_send()
    wait_halo(dirn, DEEP, start_send.at[4], start_recv.at[4])
    wait_halo(grad, DEEP, start_send.at[0], start_recv.at[0])

    @pl.loop(0, ex)
    def _(i):
        for h in range(parts):
            onward = grad[i, h] + beta * dirn[i, h]
            dirn[i, h] = onward
            gain[i, h] = csq[i, h] * onward
            adj[1, i, h] = gain[i, h] * back[1, i, h]

    def sample(s):
        @pl.loop(0, nx, unroll=2)
        def _(i):
            seen = adj[s, i + x_lo, 0, y_lo:y_hi, :] * recv_mask[i, 0]
            for h in range(1, parts):
                seen = seen + adj[s, i + x_lo, h, y_lo:y_hi, :] * recv_mask[i, h]
            value = jnp.sum(seen, axis=1, keepdims=True)
            recs[i] = jnp.where(lane[:ny] == s - 1, value, recs[i])

    out_dir = [
        pltpu.make_async_copy(src, dst, out_sem.at[0, h])
        for h, (dst, src) in enumerate(halves(dirout_h, inside(dirn)))
    ]
    sample(1)
    for copy in out_dir:
        copy.start()

    @pl.loop(0, blocks)
    def _(j):
        s = 2 * j + 1
        now, before = lax.rem(j, 2), lax.rem(j + 1, 2)

        @pl.when(j > 0)
        def _():
            wait_halo(adj.at[s], DEEP, halo_send.at[2, before], halo_recv.at[2, before])

        advance(adj, s, scattered, halo_send.at[2, now], halo_recv.at[2, now])
        sample(s + 1)
        sample(s + 2)

    wait_halo(adj.at[end], DEEP, halo_send.at[2, final], halo_recv.at[2, final])
    planes(adj, end, x_lo, x_hi, False, scattered(end))
    sample(end + 1)

    lane_r = lane[:ny]
    told = lane_r < live_here
    kept = lane_r < steps

    def score(i, sums):
        rec = jnp.where(told, recs[i], 0.0)
        res = jnp.where(kept, traces[i + x_lo, 0, y_lo:y_hi, :], 0.0)
        recs[i] = rec
        added = [fold(a * b) for a, b in ((rec, rec), (rec, res), (res, res))]
        return tuple(s + p for s, p in zip(sums, added))

    sums = lax.fori_loop(0, nx, score, (zero,) * 3)
    stacked = pack(sums)
    stacked = all_sum(stacked, slots_a.at[1], gx, gxs, gx_member, 2)
    stacked = all_sum(stacked, slots_b.at[1], place, gy_core, side_member, 3)
    upper = shot // 2
    stacked = all_sum(
        stacked, slots_c, upper, shots // 2, lambda k: {"shot": k * 2 + core}, 4
    )
    rec_sq, rec_res, res_sq = [unpack(stacked, k) for k in range(3)]
    length = slope / rec_sq

    @pl.loop(0, nx)
    def _(i):
        for h in range(parts):
            refl[i, h] = refl[i, h] + length * dirn[i + x_lo, h, y_lo:y_hi, :]

    out_image = [
        pltpu.make_async_copy(src, dst, out_sem.at[1, h])
        for h, (dst, src) in enumerate(halves(image_h, refl))
    ]
    for copy in out_image:
        copy.start()

    @pl.loop(0, nx)
    def _(i):
        recs[i] = traces[i + x_lo, 0, y_lo:y_hi, :] - length * recs[i]

    out_resid = pltpu.make_async_copy(recs, resid_h, out_sem.at[2, 0])
    out_resid.start()
    misfit = res_sq - 2.0 * length * rec_res + length * length * rec_sq
    misfit_o[...] = jnp.broadcast_to(misfit * (0.5 / entries), (8, 128))
    for copy in out_dir + out_image:
        copy.wait()
    out_resid.wait()


def on_device(groups, *arguments):
    (now, prev, csq, refl, dirn, oldg, residual, depth, source, wavelet, live) = arguments
    now, prev = now[0], prev[0]
    nx, ny, nz = now.shape
    steps = residual.shape[1]
    entries = float(residual.size * groups[0] * groups[1] * groups[2])
    ex, ey = nx + 2 * DEEP, ny + 2 * TILE
    traces = jnp.concatenate([residual[0], depth.astype(F32)], axis=0)
    traces = jnp.pad(jnp.transpose(traces, (1, 2, 0)), ((0, 0), (0, 0), (0, 127 - steps)))
    whole = pl.BlockSpec(memory_space=pl.ANY)
    small = pl.BlockSpec(memory_space=pltpu.SMEM)
    parts = nz // LANES
    grow = pltpu.VMEM((ex, parts, ey, LANES), F32)
    block = pltpu.VMEM((nx, parts, ny, LANES), F32)
    piece = pltpu.VMEM((nx // 2, parts, ny, LANES), F32)
    history = pltpu.VMEM((steps + 1, ex, parts, ey, LANES), F32)
    dma = pltpu.SemaphoreType.DMA
    image, onward, resid, misfit = pl.pallas_call(
        functools.partial(kernel, (nx, ny, nz, steps, entries), groups),
        out_shape=(
            jax.ShapeDtypeStruct((nx, ny, nz), F32),
            jax.ShapeDtypeStruct((nx, ny, nz), F32),
            jax.ShapeDtypeStruct((nx, ny, 128), F32),
            jax.ShapeDtypeStruct((8, 128), F32),
        ),
        in_specs=[whole] * 7 + [small] * 3,
        out_specs=(whole, whole, whole, pl.BlockSpec(memory_space=pltpu.VMEM)),
        scratch_shapes=[
            history,
            history,
            grow,
            grow,
            grow,
            grow,
            grow,
            grow,
            grow,
            pltpu.VMEM((nx, ny, LANES), F32),
            block,
            pltpu.VMEM((ex, 1, ey, LANES), F32),
            block,
            block,
            piece,
            piece,
            piece,
            pltpu.VMEM((2, groups[1], 8, LANES), F32),
            pltpu.VMEM((2, groups[2] * 2, 8, LANES), F32),
            pltpu.VMEM((groups[0] // 2, 8, LANES), F32),
            dma((7, parts)),
            dma((5, 8)),
            dma((5, 8)),
            dma((3, 2, 8)),
            dma((3, 2, 8)),
            dma((3,)),
            dma((3,)),
            dma((5, 8)),
            dma((5, 8)),
            dma((3, parts)),
        ],
        compiler_params=pltpu.CompilerParams(
            has_side_effects=True, vmem_limit_bytes=62 * 1024 * 1024
        ),
        name="iteration",
    )(now, prev, csq, refl, dirn, oldg, traces, source, wavelet, live)
    resid = jnp.transpose(resid[:, :, :steps], (2, 0, 1))[None]
    return image, onward, resid, misfit[0, 0]


def solution(mesh):
    groups = (mesh.shape["shot"], mesh.shape["gx"], mesh.shape["gy"])
    space = P("gx", "gy", None)
    placed = (
        P("shot", "gx", "gy", None),
        P("shot", "gx", "gy", None),
        space,
        space,
        space,
        space,
        P("shot", None, "gx", "gy"),
        P("shot", "gx", "gy"),
        P("shot", None),
        P("shot", None),
        P("shot"),
    )
    return jax.shard_map(
        functools.partial(on_device, groups),
        mesh=mesh,
        in_specs=placed,
        out_specs=(space, space, P("shot", None, "gx", "gy"), P()),
        check_vma=False,
    )
```

```python
import functools

import jax
import jax.numpy as jnp
from jax import lax
from jax.experimental import pallas as pl
from jax.experimental.pallas import tpu as pltpu
from jax.sharding import PartitionSpec as P

MESH = pl.DeviceIdType.MESH
F32 = jnp.float32
WAYS = [(-1, 0), (1, 0), (0, -1), (0, 1), (-1, -1), (-1, 1), (1, -1), (1, 1)]
DEEP = 2
TILE = 8
LANES = 128


def kernel(
    sizes,
    groups,
    now_h,
    prev_h,
    csq_h,
    refl_h,
    dirn_h,
    oldg_h,
    res_h,
    depth_h,
    source,
    wavelet,
    live,
    image_h,
    dirout_h,
    resid_h,
    misfit_o,
    back,
    adj,
    csq,
    dirn,
    grad,
    gain,
    spot,
    crec,
    twice,
    recs,
    recv_mask,
    traces,
    weights,
    csq_s,
    now_s,
    prev_s,
    dirn_s,
    oldg,
    refl,
    res_s,
    depth_s,
    resid_s,
    half_a,
    half_b,
    half_c,
    slots_a,
    slots_b,
    slots_c,
    local_sem,
    start_send,
    start_recv,
    halo_send,
    halo_recv,
    pair_send,
    pair_recv,
    sum_send,
    sum_recv,
    out_sem,
):
    nx, ny, nz, steps, entries = sizes
    shots, gxs, gys = groups
    parts = nz // LANES
    ex, ey = nx + 2 * DEEP, ny + 2 * TILE
    x_lo, x_hi = DEEP, DEEP + nx
    y_lo, y_hi = TILE, TILE + ny
    shot, gx, gy = lax.axis_index("shot"), lax.axis_index("gx"), lax.axis_index("gy")
    core = lax.rem(shot, 2)

    def has(way):
        at_x, at_y = gx + way[0], gy + way[1]
        return (at_x >= 0) & (at_x < gxs) & (at_y >= 0) & (at_y < gys)

    def regions(way, width):
        dx, dy = way
        src_x, dst_x = {
            -1: ((x_lo, width), (x_hi, width)),
            1: ((x_hi - width, width), (x_lo - width, width)),
            0: ((x_lo, nx), (x_lo, nx)),
        }[dx]
        src_y, dst_y = {
            -1: ((y_lo, TILE), (y_hi, TILE)),
            1: ((y_hi - TILE, TILE), (0, TILE)),
            0: ((y_lo, ny), (y_lo, ny)),
        }[dy]
        return (
            (pl.ds(*src_x), slice(None), pl.ds(*src_y), slice(None)),
            (pl.ds(*dst_x), slice(None), pl.ds(*dst_y), slice(None)),
        )

    def halo_copy(ref, k, width, send, recv):
        src, dst = regions(WAYS[k], width)
        return pltpu.make_async_remote_copy(
            src_ref=ref.at[src],
            dst_ref=ref.at[dst],
            send_sem=send.at[k],
            recv_sem=recv.at[k],
            device_id={"gx": gx + WAYS[k][0], "gy": gy + WAYS[k][1]},
            device_id_type=MESH,
        )

    def start_way(ref, k, width, send, recv):
        @pl.when(has(WAYS[k]))
        def _():
            halo_copy(ref, k, width, send, recv).start()

    def start_halo(ref, width, send, recv):
        for k in range(8):
            start_way(ref, k, width, send, recv)

    def wait_halo(ref, width, send, recv):
        for k, way in enumerate(WAYS):
            came = has((-way[0], -way[1]))

            @pl.when(came)
            def _():
                halo_copy(ref, k, width, send, recv).wait_recv()

            @pl.when(jnp.logical_not(came))
            def _():
                where = regions(way, width)[1]
                view = ref.at[where]
                view[...] = jnp.zeros(view.shape, F32)

            @pl.when(has(way))
            def _():
                halo_copy(ref, k, width, send, recv).wait_send()

    xs, ys = pl.ds(x_lo, nx), pl.ds(y_lo, ny)

    loads = [
        (res_h, res_s),
        (depth_h, depth_s),
        (csq_h, csq_s),
        (now_h, now_s),
        (prev_h, prev_s),
        (dirn_h, dirn_s),
        (oldg_h, oldg),
        (refl_h, refl),
    ]
    copies = [
        pltpu.make_async_copy(src, dst, local_sem.at[i]) for i, (src, dst) in enumerate(loads)
    ]
    for copy in copies:
        copy.start()

    half = nx // 2
    gy_core = gys * 2
    place = gy * 2 + core
    partner = {"shot": shot + 1 - 2 * core}
    opposite = {"shot": lax.rem(shot + 2, shots)}

    def gx_member(k):
        return {"gx": k}

    def side_member(k):
        return {"gy": k // 2, "shot": shot - core + lax.rem(k, 2)}

    barrier = pltpu.get_barrier_semaphore()

    def greet(device):
        pl.semaphore_signal(barrier, inc=1, device_id=device, device_id_type=MESH)

    for o in range(1, gxs):
        greet(gx_member(lax.rem(gx + o, gxs)))
    for o in range(1, gy_core):
        greet(side_member(lax.rem(place + o, gy_core)))
    greet(opposite)
    met = jnp.int32(gxs + gy_core - 1)
    for way in WAYS[4:]:

        @pl.when(has(way))
        def _():
            greet({"gx": gx + way[0], "gy": gy + way[1]})

        met = met + has(way).astype(jnp.int32)

    lane = lax.broadcasted_iota(jnp.int32, (ey, LANES), 1)
    row = lax.broadcasted_iota(jnp.int32, (ey, LANES), 0)
    live_here = live[0]

    @pl.loop(0, ex)
    def _(i):
        for h in range(parts):
            adj[0, i, h] = jnp.zeros((ey, LANES), F32)
            hit = (row + (gy * ny - TILE) == source[0, 1]) & (lane + h * LANES == source[0, 2])
            hit = hit & (row * 0 + (i + gx * nx - DEEP) == source[0, 0])
            spot[i, h] = jnp.where(hit, 1.0, 0.0)

    recs[...] = jnp.zeros(recs.shape, F32)

    def unpack_rows(source_ref, target):
        for i in range(nx):
            for h in range(parts):
                target[i + x_lo, h, y_lo:y_hi, :] = source_ref[i, :, h * LANES : (h + 1) * LANES]

    starts = [(traces, DEEP), (csq, DEEP), (back.at[1], DEEP), (back.at[0], 1), (dirn, DEEP)]

    def start_first(i):
        start_halo(starts[i][0], starts[i][1], start_send.at[i], start_recv.at[i])

    copies[0].wait()
    copies[1].wait()
    depths = depth_s[...].astype(F32)
    top = lax.broadcasted_iota(jnp.int32, (8, ny), 0)
    for i in range(nx):
        level = jnp.where(top == 0, depths[i : i + 1], 0.0)
        rest = jnp.zeros((LANES - steps - 8, ny), F32)
        stack = jnp.concatenate([res_s[:, i, :], level, rest], axis=0)
        traces[i + x_lo, 0, y_lo:y_hi, :] = jnp.transpose(stack)
    pl.semaphore_wait(barrier, met)
    start_first(0)
    copies[2].wait()
    unpack_rows(csq_s, csq.at[...])
    start_first(1)
    copies[3].wait()
    unpack_rows(now_s, back.at[1])
    start_first(2)
    copies[4].wait()
    unpack_rows(prev_s, back.at[0])
    start_first(3)
    copies[5].wait()
    unpack_rows(dirn_s, dirn.at[...])
    copies[6].wait()
    copies[7].wait()

    wait_halo(traces, DEEP, start_send.at[0], start_recv.at[0])

    def column(i, n, r, count):
        at = lane[:count]
        picked = jnp.where((at == n) & (at < live_here), traces[i, 0, r : r + count, :], 0.0)
        return jnp.sum(picked, axis=1, keepdims=True)

    def receivers(i):
        level = jnp.sum(jnp.where(lane == steps, traces[i, 0], 0.0), axis=1, keepdims=True)
        return [(lane + h * LANES).astype(F32) == level for h in range(parts)]

    @pl.loop(0, ex)
    def _(i):
        for n in range(steps):
            weights[n, i] = jnp.broadcast_to(column(i, n, 0, ey), (ey, LANES))

    wait_halo(csq, DEEP, start_send.at[1], start_recv.at[1])

    @pl.loop(0, ex)
    def _(i):
        for h, here in enumerate(receivers(i)):
            crec[i, h] = jnp.where(here, csq[i, h], 0.0)
            adj[1, i, h] = crec[i, h] * weights[steps - 1, i]
            twice[i, h] = 2.0 - 6.0 * csq[i, h]

    @pl.loop(0, nx)
    def _(i):
        for h, here in enumerate(receivers(i + x_lo)):
            recv_mask[i, h] = jnp.where(here, 1.0, 0.0)[y_lo:y_hi]

    def strip(field, s, i, r, count, extra):
        at = lane[:count]
        first, last = at == 0, at == LANES - 1
        rows = pl.ds(r, count)
        mids = [field[s, i, h, rows, :] for h in range(parts)]
        ups = [pltpu.roll(mid, 1, 1) for mid in mids]
        downs = [pltpu.roll(mid, LANES - 1, 1) for mid in mids]
        for h, mid in enumerate(mids):
            before = ups[h - 1] if h > 0 else 0.0
            after = downs[h + 1] if h < parts - 1 else 0.0
            left = jnp.where(first, before, ups[h])
            right = jnp.where(last, after, downs[h])
            if r > 0:
                above = field[s, i, h, pl.ds(r - 1, count), :]
            else:
                above = pltpu.roll(mid, 1, 0)
            if r + count < ey:
                below = field[s, i, h, pl.ds(r + 1, count), :]
            else:
                below = pltpu.roll(mid, count - 1, 0)
            total = (field[s, i - 1, h, rows, :] + field[s, i + 1, h, rows, :]) + (above + below)
            total = total + (left + right)
            value = csq[i, h, rows, :] * total + twice[i, h, rows, :] * mid
            value = value - field[s - 1, i, h, rows, :] + extra(i, h, r, count)
            field[s + 1, i, h, rows, :] = value

    def plane(field, s, i, whole, extra):
        if whole:
            strip(field, s, i, 0, TILE, extra)
        strip(field, s, i, y_lo, ny, extra)
        if whole:
            strip(field, s, i, y_hi, TILE, extra)

    def planes(field, s, lo, hi, whole, extra):
        @pl.loop(lo, hi, unroll=2)
        def _(i):
            plane(field, s, i, whole, extra)

    def ahead(s):
        amount = wavelet[0, s - 1]
        return lambda i, h, r, count: amount * spot[i, h, r : r + count, :]

    def behind(s):
        n = steps - 1 - s
        return lambda i, h, r, count: crec[i, h, r : r + count, :] * weights[n, i, r : r + count, :]

    def scattered(s):
        return lambda i, h, r, count: (
            gain[i, h, r : r + count, :] * back[s + 1, i, h, r : r + count, :]
        )

    def advance(field, s, make, send, recv):
        first, second = make(s), make(s + 1)
        target = field.at[s + 2]
        planes(field, s, x_lo - 1, x_lo + DEEP + 1, True, first)
        planes(field, s + 1, x_lo, x_lo + DEEP, False, second)
        start_way(target, 0, DEEP, send, recv)
        planes(field, s, x_hi - DEEP - 1, x_hi + 1, True, first)
        planes(field, s + 1, x_hi - DEEP, x_hi, False, second)
        start_way(target, 1, DEEP, send, recv)
        for k in range(4, 8):
            start_way(target, k, DEEP, send, recv)
        planes(field, s, x_lo + DEEP + 1, x_hi - DEEP - 1, True, first)
        planes(field, s + 1, x_lo + DEEP, x_hi - DEEP, False, second)
        start_way(target, 2, DEEP, send, recv)
        start_way(target, 3, DEEP, send, recv)

    blocks = (steps - 1) // 2

    @pl.loop(0, blocks)
    def _(j):
        s = 2 * j + 1
        now, before = lax.rem(j, 2), lax.rem(j + 1, 2)
        for field, way, make in ((adj, 1, behind), (back, 0, ahead)):

            @pl.when(j > 0)
            def _():
                wait_halo(field.at[s], DEEP, halo_send.at[way, before], halo_recv.at[way, before])

            if way == 0:

                @pl.when(j == 0)
                def _():
                    wait_halo(back.at[1], DEEP, start_send.at[2], start_recv.at[2])
                    wait_halo(back.at[0], 1, start_send.at[3], start_recv.at[3])

            advance(field, s, make, halo_send.at[way, now], halo_recv.at[way, now])

    end = 2 * blocks + 1
    final = (blocks - 1) % 2
    for field, way, make in ((adj, 1, behind), (back, 0, ahead)):
        wait_halo(field.at[end], DEEP, halo_send.at[way, final], halo_recv.at[way, final])
        planes(field, end, x_lo, x_hi, False, make(end))

    start_first(4)

    mine, other = x_lo + half * core, x_lo + half * (1 - core)
    own_half = (pl.ds(mine, half), slice(None), ys, slice(None))

    def products(start, keep):
        @pl.loop(start, start + half)
        def _(i):
            for h in range(parts):
                total = back[1, i, h, y_lo:y_hi, :] * adj[steps, i, h, y_lo:y_hi, :]
                for a in range(2, steps + 1):
                    one, two = back[a, i, h, y_lo:y_hi, :], adj[steps + 1 - a, i, h, y_lo:y_hi, :]
                    total = total + one * two
                keep(i, h, total)

    def pair_copy(src, dst, k, device):
        return pltpu.make_async_remote_copy(
            src_ref=src,
            dst_ref=dst,
            send_sem=pair_send.at[k],
            recv_sem=pair_recv.at[k],
            device_id=device,
            device_id_type=MESH,
        )

    def keep_other(i, h, total):
        half_c[i - other, h] = total

    def keep_mine(i, h, total):
        grad[i, h, y_lo:y_hi, :] = total

    products(other, keep_other)
    swap_a = pair_copy(half_c, half_a, 0, partner)
    swap_a.start()
    products(mine, keep_mine)
    swap_a.wait()

    def add_half(buffer):
        @pl.loop(0, half)
        def _(i):
            for h in range(parts):
                was = grad[mine + i, h, y_lo:y_hi, :]
                grad[mine + i, h, y_lo:y_hi, :] = was + buffer[i, h]

    add_half(half_a)
    swap_b = pair_copy(grad.at[own_half], half_b, 1, opposite)
    swap_b.start()
    swap_b.wait()
    add_half(half_b)
    spread = pair_copy(grad.at[own_half], grad.at[own_half], 2, partner)
    spread.start()

    def fold(values):
        return jnp.sum(values.reshape(-1, 8, LANES), axis=0)

    def dots(i, sums):
        for h in range(parts):
            g = grad[mine + i, h, y_lo:y_hi, :]
            o = oldg[mine + i - x_lo, :, h * LANES : (h + 1) * LANES]
            d = dirn[mine + i, h, y_lo:y_hi, :]
            added = [fold(a * b) for a, b in ((g, g), (g, o), (o, o), (g, d))]
            sums = tuple(s + p for s, p in zip(sums, added))
        return sums

    zero = jnp.zeros((8, LANES), F32)
    eight = lax.broadcasted_iota(jnp.int32, (8, LANES), 0)

    def pack(sums):
        packed = zero
        for k, value in enumerate(sums):
            packed = jnp.where(eight == k, jnp.sum(value, axis=0, keepdims=True), packed)
        return packed

    def unpack(packed, k):
        return jnp.sum(packed[k : k + 1], axis=1, keepdims=True)

    sums = lax.fori_loop(0, half, dots, (zero,) * 4)
    def all_sum(values, slots, at, count, member, base):
        slots[at] = values

        def copy(peer, slot):
            return pltpu.make_async_remote_copy(
                src_ref=slots.at[at],
                dst_ref=slots.at[slot],
                send_sem=sum_send.at[base, peer],
                recv_sem=sum_recv.at[base, slot],
                device_id=member(peer),
                device_id_type=MESH,
            )

        for o in range(1, count):
            copy(lax.rem(at + o, count), at).start()
        for o in range(1, count):
            source_at = lax.rem(at + count - o, count)
            copy(source_at, source_at).wait_recv()
        for o in range(1, count):
            copy(lax.rem(at + o, count), at).wait_send()
        total = slots[0]
        for k in range(1, count):
            total = total + slots[k]
        return total

    stacked = pack(sums)
    spread.wait_recv()
    start_halo(grad, DEEP, start_send.at[0], start_recv.at[0])
    stacked = all_sum(stacked, slots_a.at[0], gx, gxs, gx_member, 0)
    stacked = all_sum(stacked, slots_b.at[0], place, gy_core, side_member, 1)
    grad_sq, cross, old_sq, toward = [unpack(stacked, k) for k in range(4)]
    beta = (grad_sq - cross) / old_sq
    slope = grad_sq + beta * toward
    spread.wait_send()
    wait_halo(dirn, DEEP, start_send.at[4], start_recv.at[4])
    wait_halo(grad, DEEP, start_send.at[0], start_recv.at[0])

    @pl.loop(0, ex)
    def _(i):
        for h in range(parts):
            onward = grad[i, h] + beta * dirn[i, h]
            dirn[i, h] = onward
            gain[i, h] = csq[i, h] * onward
            adj[1, i, h] = gain[i, h] * back[1, i, h]

    def sample(s):
        @pl.loop(0, nx, unroll=2)
        def _(i):
            seen = adj[s, i + x_lo, 0, y_lo:y_hi, :] * recv_mask[i, 0]
            for h in range(1, parts):
                seen = seen + adj[s, i + x_lo, h, y_lo:y_hi, :] * recv_mask[i, h]
            value = jnp.sum(seen, axis=1, keepdims=True)
            recs[i] = jnp.where(lane[:ny] == s - 1, value, recs[i])

    @pl.loop(0, nx)
    def _(i):
        for h in range(parts):
            dirn_s[i, :, h * LANES : (h + 1) * LANES] = dirn[i + x_lo, h, y_lo:y_hi, :]

    out_dir = pltpu.make_async_copy(dirn_s, dirout_h, out_sem.at[0])
    out_dir.start()
    sample(1)

    @pl.loop(0, blocks)
    def _(j):
        s = 2 * j + 1
        now, before = lax.rem(j, 2), lax.rem(j + 1, 2)

        @pl.when(j > 0)
        def _():
            wait_halo(adj.at[s], DEEP, halo_send.at[2, before], halo_recv.at[2, before])

        advance(adj, s, scattered, halo_send.at[2, now], halo_recv.at[2, now])
        sample(s + 1)
        sample(s + 2)

    wait_halo(adj.at[end], DEEP, halo_send.at[2, final], halo_recv.at[2, final])
    planes(adj, end, x_lo, x_hi, False, scattered(end))
    sample(end + 1)

    lane_r = lane[:ny]
    told = lane_r < live_here
    kept = lane_r < steps

    def score(i, sums):
        rec = jnp.where(told, recs[i], 0.0)
        res = jnp.where(kept, traces[i + x_lo, 0, y_lo:y_hi, :], 0.0)
        recs[i] = rec
        added = [fold(a * b) for a, b in ((rec, rec), (rec, res), (res, res))]
        return tuple(s + p for s, p in zip(sums, added))

    sums = lax.fori_loop(0, nx, score, (zero,) * 3)
    stacked = pack(sums)
    stacked = all_sum(stacked, slots_a.at[1], gx, gxs, gx_member, 2)
    stacked = all_sum(stacked, slots_b.at[1], place, gy_core, side_member, 3)
    upper = shot // 2
    stacked = all_sum(
        stacked, slots_c, upper, shots // 2, lambda k: {"shot": k * 2 + core}, 4
    )
    rec_sq, rec_res, res_sq = [unpack(stacked, k) for k in range(3)]
    length = slope / rec_sq

    @pl.loop(0, nx)
    def _(i):
        for h in range(parts):
            span = slice(h * LANES, (h + 1) * LANES)
            refl[i, :, span] = refl[i, :, span] + length * dirn[i + x_lo, h, y_lo:y_hi, :]

    out_image = pltpu.make_async_copy(refl, image_h, out_sem.at[1])
    out_image.start()
    for i in range(nx):
        rest = traces[i + x_lo, 0, y_lo:y_hi, :] - length * recs[i]
        resid_s[:, i, :] = jnp.transpose(rest)[:steps]

    out_resid = pltpu.make_async_copy(resid_s, resid_h, out_sem.at[2])
    out_resid.start()
    misfit = res_sq - 2.0 * length * rec_res + length * length * rec_sq
    misfit_o[...] = jnp.broadcast_to(misfit * (0.5 / entries), (8, 128))
    out_dir.wait()
    out_image.wait()
    out_resid.wait()


def on_device(groups, *arguments):
    (now, prev, csq, refl, dirn, oldg, residual, depth, source, wavelet, live) = arguments
    now, prev = now[0], prev[0]
    nx, ny, nz = now.shape
    steps = residual.shape[1]
    entries = float(residual.size * groups[0] * groups[1] * groups[2])
    ex, ey = nx + 2 * DEEP, ny + 2 * TILE
    whole = pl.BlockSpec(memory_space=pl.ANY)
    small = pl.BlockSpec(memory_space=pltpu.SMEM)
    parts = nz // LANES
    grow = pltpu.VMEM((ex, parts, ey, LANES), F32)
    block = pltpu.VMEM((nx, parts, ny, LANES), F32)
    stage = pltpu.VMEM((nx, ny, nz), F32)
    piece = pltpu.VMEM((nx // 2, parts, ny, LANES), F32)
    history = pltpu.VMEM((steps + 1, ex, parts, ey, LANES), F32)
    dma = pltpu.SemaphoreType.DMA
    image, onward, resid, misfit = pl.pallas_call(
        functools.partial(kernel, (nx, ny, nz, steps, entries), groups),
        out_shape=(
            jax.ShapeDtypeStruct((nx, ny, nz), F32),
            jax.ShapeDtypeStruct((nx, ny, nz), F32),
            jax.ShapeDtypeStruct((steps, nx, ny), F32),
            jax.ShapeDtypeStruct((8, 128), F32),
        ),
        in_specs=[whole] * 8 + [small] * 3,
        out_specs=(whole, whole, whole, pl.BlockSpec(memory_space=pltpu.VMEM)),
        scratch_shapes=[
            history,
            history,
            grow,
            grow,
            grow,
            grow,
            grow,
            grow,
            grow,
            pltpu.VMEM((nx, ny, LANES), F32),
            block,
            pltpu.VMEM((ex, 1, ey, LANES), F32),
            pltpu.VMEM((steps, ex, ey, LANES), F32),
            stage,
            stage,
            stage,
            stage,
            stage,
            stage,
            pltpu.VMEM((steps, nx, ny), F32),
            pltpu.VMEM((nx, ny), jnp.int32),
            pltpu.VMEM((steps, nx, ny), F32),
            piece,
            piece,
            piece,
            pltpu.VMEM((2, groups[1], 8, LANES), F32),
            pltpu.VMEM((2, groups[2] * 2, 8, LANES), F32),
            pltpu.VMEM((groups[0] // 2, 8, LANES), F32),
            dma((8,)),
            dma((5, 8)),
            dma((5, 8)),
            dma((3, 2, 8)),
            dma((3, 2, 8)),
            dma((3,)),
            dma((3,)),
            dma((5, 8)),
            dma((5, 8)),
            dma((3,)),
        ],
        compiler_params=pltpu.CompilerParams(
            has_side_effects=True, collective_id=0, vmem_limit_bytes=62 * 1024 * 1024
        ),
        name="iteration",
    )(now, prev, csq, refl, dirn, oldg, residual[0], depth[0], source, wavelet, live)
    return image, onward, resid[None], misfit[0, 0]


def solution(mesh):
    groups = (mesh.shape["shot"], mesh.shape["gx"], mesh.shape["gy"])
    space = P("gx", "gy", None)
    placed = (
        P("shot", "gx", "gy", None),
        P("shot", "gx", "gy", None),
        space,
        space,
        space,
        space,
        P("shot", None, "gx", "gy"),
        P("shot", "gx", "gy"),
        P("shot", None),
        P("shot", None),
        P("shot"),
    )
    return jax.shard_map(
        functools.partial(on_device, groups),
        mesh=mesh,
        in_specs=placed,
        out_specs=(space, space, P("shot", None, "gx", "gy"), P()),
        check_vma=False,
    )
```

```python
import functools

import jax
import jax.numpy as jnp
from jax import lax
from jax.experimental import pallas as pl
from jax.experimental.pallas import tpu as pltpu
from jax.sharding import PartitionSpec as P

MESH = pl.DeviceIdType.MESH
F32 = jnp.float32
WAYS = [(-1, 0), (1, 0), (0, -1), (0, 1), (-1, -1), (-1, 1), (1, -1), (1, 1)]
DEEP = 2
TILE = 8
LANES = 128


def kernel(
    sizes,
    groups,
    now_h,
    prev_h,
    csq_h,
    dirn_h,
    oldg_h,
    res_h,
    depth_h,
    source,
    wavelet,
    live,
    grad_h,
    born_h,
    scalars_o,
    back,
    adj,
    csq,
    dirn,
    grad,
    gain,
    spot,
    crec,
    twice,
    recs,
    recv_mask,
    traces,
    weights,
    csq_s,
    now_s,
    prev_s,
    dirn_s,
    oldg,
    res_s,
    depth_s,
    resid_s,
    half_a,
    half_b,
    half_c,
    slots_a,
    slots_b,
    slots_c,
    local_sem,
    start_send,
    start_recv,
    halo_send,
    halo_recv,
    pair_send,
    pair_recv,
    sum_send,
    sum_recv,
    out_sem,
):
    nx, ny, nz, steps, entries = sizes
    shots, gxs, gys = groups
    parts = nz // LANES
    ex, ey = nx + 2 * DEEP, ny + 2 * TILE
    x_lo, x_hi = DEEP, DEEP + nx
    y_lo, y_hi = TILE, TILE + ny
    shot, gx, gy = lax.axis_index("shot"), lax.axis_index("gx"), lax.axis_index("gy")
    core = lax.rem(shot, 2)

    def has(way):
        at_x, at_y = gx + way[0], gy + way[1]
        return (at_x >= 0) & (at_x < gxs) & (at_y >= 0) & (at_y < gys)

    def regions(way, width):
        dx, dy = way
        src_x, dst_x = {
            -1: ((x_lo, width), (x_hi, width)),
            1: ((x_hi - width, width), (x_lo - width, width)),
            0: ((x_lo, nx), (x_lo, nx)),
        }[dx]
        src_y, dst_y = {
            -1: ((y_lo, TILE), (y_hi, TILE)),
            1: ((y_hi - TILE, TILE), (0, TILE)),
            0: ((y_lo, ny), (y_lo, ny)),
        }[dy]
        return (
            (pl.ds(*src_x), slice(None), pl.ds(*src_y), slice(None)),
            (pl.ds(*dst_x), slice(None), pl.ds(*dst_y), slice(None)),
        )

    def halo_copy(ref, k, width, send, recv):
        src, dst = regions(WAYS[k], width)
        return pltpu.make_async_remote_copy(
            src_ref=ref.at[src],
            dst_ref=ref.at[dst],
            send_sem=send.at[k],
            recv_sem=recv.at[k],
            device_id={"gx": gx + WAYS[k][0], "gy": gy + WAYS[k][1]},
            device_id_type=MESH,
        )

    def start_way(ref, k, width, send, recv):
        @pl.when(has(WAYS[k]))
        def _():
            halo_copy(ref, k, width, send, recv).start()

    def start_halo(ref, width, send, recv):
        for k in (4, 5, 6, 7, 0, 1, 2, 3):
            start_way(ref, k, width, send, recv)

    def wait_halo(ref, width, send, recv):
        for k, way in enumerate(WAYS):
            came = has((-way[0], -way[1]))

            @pl.when(came)
            def _():
                halo_copy(ref, k, width, send, recv).wait_recv()

            @pl.when(jnp.logical_not(came))
            def _():
                where = regions(way, width)[1]
                view = ref.at[where]
                view[...] = jnp.zeros(view.shape, F32)

            @pl.when(has(way))
            def _():
                halo_copy(ref, k, width, send, recv).wait_send()

    xs, ys = pl.ds(x_lo, nx), pl.ds(y_lo, ny)

    loads = [
        (res_h, res_s),
        (depth_h, depth_s),
        (csq_h, csq_s),
        (now_h, now_s),
        (prev_h, prev_s),
        (dirn_h, dirn_s),
        (oldg_h, oldg),
    ]
    copies = [
        pltpu.make_async_copy(src, dst, local_sem.at[i]) for i, (src, dst) in enumerate(loads)
    ]
    for copy in copies:
        copy.start()

    half = nx // 2
    gy_core = gys * 2
    place = gy * 2 + core
    partner = {"shot": shot + 1 - 2 * core}
    opposite = {"shot": lax.rem(shot + 2, shots)}

    def gx_member(k):
        return {"gx": k}

    def side_member(k):
        return {"gy": k // 2, "shot": shot - core + lax.rem(k, 2)}

    wide = gy * shots + shot

    def wide_member(k):
        return {"gy": k // shots, "shot": lax.rem(k, shots)}

    barrier = pltpu.get_barrier_semaphore()

    def greet(device):
        pl.semaphore_signal(barrier, inc=1, device_id=device, device_id_type=MESH)

    for o in range(1, gxs):
        greet(gx_member(lax.rem(gx + o, gxs)))
    for o in range(1, gys * shots):
        greet(wide_member(lax.rem(wide + o, gys * shots)))
    met = jnp.int32(gxs + gys * shots - 2)
    for way in WAYS[4:]:

        @pl.when(has(way))
        def _():
            greet({"gx": gx + way[0], "gy": gy + way[1]})

        met = met + has(way).astype(jnp.int32)

    lane = lax.broadcasted_iota(jnp.int32, (ey, LANES), 1)
    row = lax.broadcasted_iota(jnp.int32, (ey, LANES), 0)
    live_here = live[0]

    @pl.loop(0, ex)
    def _(i):
        for h in range(parts):
            adj[0, i, h] = jnp.zeros((ey, LANES), F32)
            hit = (row + (gy * ny - TILE) == source[0, 1]) & (lane + h * LANES == source[0, 2])
            hit = hit & (row * 0 + (i + gx * nx - DEEP) == source[0, 0])
            spot[i, h] = jnp.where(hit, 1.0, 0.0)

    recs[...] = jnp.zeros(recs.shape, F32)

    def unpack_rows(source_ref, target):
        for i in range(nx):
            for h in range(parts):
                target[i + x_lo, h, y_lo:y_hi, :] = source_ref[i, :, h * LANES : (h + 1) * LANES]

    starts = [(traces, DEEP), (csq, DEEP), (back.at[1], DEEP), (back.at[0], 1), (dirn, DEEP)]

    def start_first(i):
        start_halo(starts[i][0], starts[i][1], start_send.at[i], start_recv.at[i])

    copies[0].wait()
    copies[1].wait()
    depths = depth_s[...].astype(F32)
    top = lax.broadcasted_iota(jnp.int32, (8, ny), 0)
    for i in range(nx):
        level = jnp.where(top == 0, depths[i : i + 1], 0.0)
        rest = jnp.zeros((LANES - steps - 8, ny), F32)
        stack = jnp.concatenate([res_s[:, i, :], level, rest], axis=0)
        traces[i + x_lo, 0, y_lo:y_hi, :] = jnp.transpose(stack)
    pl.semaphore_wait(barrier, met)
    start_first(0)
    copies[2].wait()
    unpack_rows(csq_s, csq.at[...])
    start_first(1)
    copies[3].wait()
    unpack_rows(now_s, back.at[1])
    start_first(2)
    copies[4].wait()
    unpack_rows(prev_s, back.at[0])
    start_first(3)
    copies[5].wait()
    unpack_rows(dirn_s, dirn.at[...])
    copies[6].wait()

    wait_halo(traces, DEEP, start_send.at[0], start_recv.at[0])

    def column(i, n, r, count):
        at = lane[:count]
        picked = jnp.where((at == n) & (at < live_here), traces[i, 0, r : r + count, :], 0.0)
        return jnp.sum(picked, axis=1, keepdims=True)

    def receivers(i):
        level = jnp.sum(jnp.where(lane == steps, traces[i, 0], 0.0), axis=1, keepdims=True)
        return [(lane + h * LANES).astype(F32) == level for h in range(parts)]

    @pl.loop(0, ex)
    def _(i):
        for n in range(steps):
            weights[n, i] = jnp.broadcast_to(column(i, n, 0, ey), (ey, LANES))

    wait_halo(csq, DEEP, start_send.at[1], start_recv.at[1])

    @pl.loop(0, ex)
    def _(i):
        for h, here in enumerate(receivers(i)):
            crec[i, h] = jnp.where(here, csq[i, h], 0.0)
            adj[1, i, h] = crec[i, h] * weights[steps - 1, i]
            twice[i, h] = 2.0 - 6.0 * csq[i, h]

    @pl.loop(0, nx)
    def _(i):
        for h, here in enumerate(receivers(i + x_lo)):
            recv_mask[i, h] = jnp.where(here, 1.0, 0.0)[y_lo:y_hi]

    def strip(field, s, i, r, count, extra):
        at = lane[:count]
        first, last = at == 0, at == LANES - 1
        rows = pl.ds(r, count)
        mids = [field[s, i, h, rows, :] for h in range(parts)]
        ups = [pltpu.roll(mid, 1, 1) for mid in mids]
        downs = [pltpu.roll(mid, LANES - 1, 1) for mid in mids]
        for h, mid in enumerate(mids):
            before = ups[h - 1] if h > 0 else 0.0
            after = downs[h + 1] if h < parts - 1 else 0.0
            left = jnp.where(first, before, ups[h])
            right = jnp.where(last, after, downs[h])
            if r > 0:
                above = field[s, i, h, pl.ds(r - 1, count), :]
            else:
                above = pltpu.roll(mid, 1, 0)
            if r + count < ey:
                below = field[s, i, h, pl.ds(r + 1, count), :]
            else:
                below = pltpu.roll(mid, count - 1, 0)
            total = (field[s, i - 1, h, rows, :] + field[s, i + 1, h, rows, :]) + (above + below)
            total = total + (left + right)
            value = csq[i, h, rows, :] * total + twice[i, h, rows, :] * mid
            value = value - field[s - 1, i, h, rows, :] + extra(i, h, r, count)
            field[s + 1, i, h, rows, :] = value

    def plane(field, s, i, whole, extra):
        if whole:
            strip(field, s, i, 0, TILE, extra)
        strip(field, s, i, y_lo, ny, extra)
        if whole:
            strip(field, s, i, y_hi, TILE, extra)

    def planes(field, s, lo, hi, whole, extra):
        @pl.loop(lo, hi, unroll=2)
        def _(i):
            plane(field, s, i, whole, extra)

    def ahead(s):
        amount = wavelet[0, s - 1]
        return lambda i, h, r, count: amount * spot[i, h, r : r + count, :]

    def behind(s):
        n = steps - 1 - s
        return lambda i, h, r, count: crec[i, h, r : r + count, :] * weights[n, i, r : r + count, :]

    def scattered(s):
        return lambda i, h, r, count: (
            gain[i, h, r : r + count, :] * back[s + 1, i, h, r : r + count, :]
        )

    def advance(field, s, make, send, recv):
        first, second = make(s), make(s + 1)
        target = field.at[s + 2]
        planes(field, s, x_lo - 1, x_lo + DEEP + 1, True, first)
        planes(field, s + 1, x_lo, x_lo + DEEP, False, second)
        for k in (4, 5, 0):
            start_way(target, k, DEEP, send, recv)
        planes(field, s, x_hi - DEEP - 1, x_hi + 1, True, first)
        planes(field, s + 1, x_hi - DEEP, x_hi, False, second)
        for k in (6, 7, 1):
            start_way(target, k, DEEP, send, recv)
        planes(field, s, x_lo + DEEP + 1, x_hi - DEEP - 1, True, first)
        planes(field, s + 1, x_lo + DEEP, x_hi - DEEP, False, second)
        start_way(target, 2, DEEP, send, recv)
        start_way(target, 3, DEEP, send, recv)

    blocks = (steps - 1) // 2

    @pl.loop(0, blocks)
    def _(j):
        s = 2 * j + 1
        now, before = lax.rem(j, 2), lax.rem(j + 1, 2)
        for field, way, make in ((adj, 1, behind), (back, 0, ahead)):

            @pl.when(j > 0)
            def _():
                wait_halo(field.at[s], DEEP, halo_send.at[way, before], halo_recv.at[way, before])

            if way == 0:

                @pl.when(j == 0)
                def _():
                    wait_halo(back.at[1], DEEP, start_send.at[2], start_recv.at[2])
                    wait_halo(back.at[0], 1, start_send.at[3], start_recv.at[3])

            advance(field, s, make, halo_send.at[way, now], halo_recv.at[way, now])

    end = 2 * blocks + 1
    final = (blocks - 1) % 2
    for field, way, make in ((adj, 1, behind), (back, 0, ahead)):
        wait_halo(field.at[end], DEEP, halo_send.at[way, final], halo_recv.at[way, final])
        planes(field, end, x_lo, x_hi, False, make(end))

    start_first(4)

    mine, other = x_lo + half * core, x_lo + half * (1 - core)

    def product(i, h):
        total = back[1, i, h, y_lo:y_hi, :] * adj[steps, i, h, y_lo:y_hi, :]
        for a in range(2, steps + 1):
            one, two = back[a, i, h, y_lo:y_hi, :], adj[steps + 1 - a, i, h, y_lo:y_hi, :]
            total = total + one * two
        return total

    def pair_copy(src, dst, k, p, device):
        return pltpu.make_async_remote_copy(
            src_ref=src,
            dst_ref=dst,
            send_sem=pair_send.at[k, p],
            recv_sem=pair_recv.at[k, p],
            device_id=device,
            device_id_type=MESH,
        )

    def own_plane(p):
        return grad.at[mine + p, :, ys, :]

    def swap_a(p):
        return pair_copy(half_c.at[p], half_a.at[p], 0, p, partner)

    def swap_b(p):
        return pair_copy(own_plane(p), half_b.at[p], 1, p, opposite)

    def spread(p):
        return pair_copy(own_plane(p), own_plane(p), 2, p, partner)

    def add_plane(p, buffer):
        for h in range(parts):
            grad[mine + p, h, y_lo:y_hi, :] = grad[mine + p, h, y_lo:y_hi, :] + buffer[p, h]

    @pl.loop(0, half)
    def _(p):
        for h in range(parts):
            half_c[p, h] = product(other + p, h)
        swap_a(p).start()

    @pl.loop(0, half)
    def _(p):
        for h in range(parts):
            grad[mine + p, h, y_lo:y_hi, :] = product(mine + p, h)
        swap_a(p).wait()
        add_plane(p, half_a)
        swap_b(p).start()

    @pl.loop(0, half)
    def _(p):
        swap_b(p).wait()
        add_plane(p, half_b)
        spread(p).start()

    def fold(values):
        return jnp.sum(values.reshape(-1, 8, LANES), axis=0)

    def dots(i, sums):
        for h in range(parts):
            g = grad[mine + i, h, y_lo:y_hi, :]
            o = oldg[mine + i - x_lo, :, h * LANES : (h + 1) * LANES]
            d = dirn[mine + i, h, y_lo:y_hi, :]
            added = [fold(a * b) for a, b in ((g, g), (g, o), (o, o), (g, d))]
            sums = tuple(s + p for s, p in zip(sums, added))
        return sums

    zero = jnp.zeros((8, LANES), F32)
    eight = lax.broadcasted_iota(jnp.int32, (8, LANES), 0)

    def pack(sums):
        packed = zero
        for k, value in enumerate(sums):
            packed = jnp.where(eight == k, jnp.sum(value, axis=0, keepdims=True), packed)
        return packed

    def unpack(packed, k):
        return jnp.sum(packed[k : k + 1], axis=1, keepdims=True)

    sums = lax.fori_loop(0, half, dots, (zero,) * 4)
    def all_sum(values, slots, at, count, member, base):
        slots[at] = values

        def copy(peer, slot):
            return pltpu.make_async_remote_copy(
                src_ref=slots.at[at],
                dst_ref=slots.at[slot],
                send_sem=sum_send.at[base, peer],
                recv_sem=sum_recv.at[base, slot],
                device_id=member(peer),
                device_id_type=MESH,
            )

        for o in range(1, count):
            copy(lax.rem(at + o, count), at).start()
        for o in range(1, count):
            source_at = lax.rem(at + count - o, count)
            copy(source_at, source_at).wait_recv()
        for o in range(1, count):
            copy(lax.rem(at + o, count), at).wait_send()
        total = slots[0]
        for k in range(1, count):
            total = total + slots[k]
        return total

    stacked = pack(sums)
    for p in range(half):
        spread(p).wait_recv()
    start_halo(grad, DEEP, start_send.at[0], start_recv.at[0])
    stacked = all_sum(stacked, slots_a.at[0], gx, gxs, gx_member, 0)
    stacked = all_sum(stacked, slots_b, place, gy_core, side_member, 1)
    grad_sq, cross, old_sq, toward = [unpack(stacked, k) for k in range(4)]
    beta = (grad_sq - cross) / old_sq
    slope = grad_sq + beta * toward
    for p in range(half):
        spread(p).wait_send()
    wait_halo(dirn, DEEP, start_send.at[4], start_recv.at[4])
    wait_halo(grad, DEEP, start_send.at[0], start_recv.at[0])

    @pl.loop(0, ex)
    def _(i):
        for h in range(parts):
            onward = grad[i, h] + beta * dirn[i, h]
            dirn[i, h] = onward
            gain[i, h] = csq[i, h] * onward
            adj[1, i, h] = gain[i, h] * back[1, i, h]

    def sample(s):
        @pl.loop(0, nx, unroll=2)
        def _(i):
            seen = adj[s, i + x_lo, 0, y_lo:y_hi, :] * recv_mask[i, 0]
            for h in range(1, parts):
                seen = seen + adj[s, i + x_lo, h, y_lo:y_hi, :] * recv_mask[i, h]
            value = jnp.sum(seen, axis=1, keepdims=True)
            recs[i] = jnp.where(lane[:ny] == s - 1, value, recs[i])

    @pl.loop(0, nx)
    def _(i):
        for h in range(parts):
            dirn_s[i, :, h * LANES : (h + 1) * LANES] = grad[i + x_lo, h, y_lo:y_hi, :]

    out_grad = pltpu.make_async_copy(dirn_s, grad_h, out_sem.at[0])
    out_grad.start()
    sample(1)

    @pl.loop(0, blocks)
    def _(j):
        s = 2 * j + 1
        now, before = lax.rem(j, 2), lax.rem(j + 1, 2)

        @pl.when(j > 0)
        def _():
            wait_halo(adj.at[s], DEEP, halo_send.at[2, before], halo_recv.at[2, before])

        advance(adj, s, scattered, halo_send.at[2, now], halo_recv.at[2, now])
        sample(s + 1)
        sample(s + 2)

    wait_halo(adj.at[end], DEEP, halo_send.at[2, final], halo_recv.at[2, final])
    planes(adj, end, x_lo, x_hi, False, scattered(end))
    sample(end + 1)

    lane_r = lane[:ny]
    told = lane_r < live_here
    kept = lane_r < steps

    def score(i, sums):
        rec = jnp.where(told, recs[i], 0.0)
        res = jnp.where(kept, traces[i + x_lo, 0, y_lo:y_hi, :], 0.0)
        recs[i] = rec
        added = [fold(a * b) for a, b in ((rec, rec), (rec, res), (res, res))]
        return tuple(s + p for s, p in zip(sums, added))

    sums = lax.fori_loop(0, nx, score, (zero,) * 3)
    for i in range(nx):
        resid_s[:, i, :] = jnp.transpose(recs[i])[:steps]

    out_born = pltpu.make_async_copy(resid_s, born_h, out_sem.at[1])
    out_born.start()
    stacked = pack(sums)
    stacked = all_sum(stacked, slots_a.at[1], gx, gxs, gx_member, 2)
    stacked = all_sum(stacked, slots_c, wide, gys * shots, wide_member, 3)
    rec_sq, rec_res, res_sq = [unpack(stacked, k) for k in range(3)]
    length = slope / rec_sq

    misfit = res_sq - 2.0 * length * rec_res + length * length * rec_sq
    scalars = jnp.where(eight == 0, beta, jnp.where(eight == 1, length, misfit * (0.5 / entries)))
    scalars_o[...] = scalars
    out_grad.wait()
    out_born.wait()


def on_device(groups, *arguments):
    (now, prev, csq, refl, dirn, oldg, residual, depth, source, wavelet, live) = arguments
    now, prev = now[0], prev[0]
    nx, ny, nz = now.shape
    steps = residual.shape[1]
    entries = float(residual.size * groups[0] * groups[1] * groups[2])
    ex, ey = nx + 2 * DEEP, ny + 2 * TILE
    whole = pl.BlockSpec(memory_space=pl.ANY)
    small = pl.BlockSpec(memory_space=pltpu.SMEM)
    parts = nz // LANES
    grow = pltpu.VMEM((ex, parts, ey, LANES), F32)
    block = pltpu.VMEM((nx, parts, ny, LANES), F32)
    stage = pltpu.VMEM((nx, ny, nz), F32)
    piece = pltpu.VMEM((nx // 2, parts, ny, LANES), F32)
    history = pltpu.VMEM((steps + 1, ex, parts, ey, LANES), F32)
    dma = pltpu.SemaphoreType.DMA
    grad, born, scalars = pl.pallas_call(
        functools.partial(kernel, (nx, ny, nz, steps, entries), groups),
        out_shape=(
            jax.ShapeDtypeStruct((nx, ny, nz), F32),
            jax.ShapeDtypeStruct((steps, nx, ny), F32),
            jax.ShapeDtypeStruct((8, 128), F32),
        ),
        in_specs=[whole] * 7 + [small] * 3,
        out_specs=(whole, whole, pl.BlockSpec(memory_space=pltpu.VMEM)),
        scratch_shapes=[
            history,
            history,
            grow,
            grow,
            grow,
            grow,
            grow,
            grow,
            grow,
            pltpu.VMEM((nx, ny, LANES), F32),
            block,
            pltpu.VMEM((ex, 1, ey, LANES), F32),
            pltpu.VMEM((steps, ex, ey, LANES), F32),
            stage,
            stage,
            stage,
            stage,
            stage,
            pltpu.VMEM((steps, nx, ny), F32),
            pltpu.VMEM((nx, ny), jnp.int32),
            pltpu.VMEM((steps, nx, ny), F32),
            piece,
            piece,
            piece,
            pltpu.VMEM((2, groups[1], 8, LANES), F32),
            pltpu.VMEM((groups[2] * 2, 8, LANES), F32),
            pltpu.VMEM((groups[2] * groups[0], 8, LANES), F32),
            dma((7,)),
            dma((5, 8)),
            dma((5, 8)),
            dma((3, 2, 8)),
            dma((3, 2, 8)),
            dma((3, nx // 2)),
            dma((3, nx // 2)),
            dma((4, 16)),
            dma((4, 16)),
            dma((2,)),
        ],
        compiler_params=pltpu.CompilerParams(
            has_side_effects=True, collective_id=0, vmem_limit_bytes=62 * 1024 * 1024
        ),
        name="iteration",
    )(now, prev, csq, dirn, oldg, residual[0], depth[0], source, wavelet, live)
    beta, length, misfit = scalars[0, 0], scalars[1, 0], scalars[2, 0]
    onward = grad + beta * dirn
    image = refl + length * onward
    return image, onward, residual - length * born[None], misfit


def solution(mesh):
    groups = (mesh.shape["shot"], mesh.shape["gx"], mesh.shape["gy"])
    space = P("gx", "gy", None)
    placed = (
        P("shot", "gx", "gy", None),
        P("shot", "gx", "gy", None),
        space,
        space,
        space,
        space,
        P("shot", None, "gx", "gy"),
        P("shot", "gx", "gy"),
        P("shot", None),
        P("shot", None),
        P("shot"),
    )
    return jax.shard_map(
        functools.partial(on_device, groups),
        mesh=mesh,
        in_specs=placed,
        out_specs=(space, space, P("shot", None, "gx", "gy"), P()),
        check_vma=False,
    )
```

```python
import functools

import jax
import jax.numpy as jnp
from jax import lax
from jax.experimental import pallas as pl
from jax.experimental.pallas import tpu as pltpu
from jax.sharding import PartitionSpec as P

MESH = pl.DeviceIdType.MESH
F32 = jnp.float32
WAYS = [(-1, 0), (1, 0), (0, -1), (0, 1), (-1, -1), (-1, 1), (1, -1), (1, 1)]
DEEP = 2
TILE = 8
LANES = 128


def kernel(
    sizes,
    groups,
    now_h,
    prev_h,
    csq_h,
    dirn_h,
    oldg_h,
    res_h,
    depth_h,
    source,
    wavelet,
    live,
    grad_h,
    born_h,
    scalars_o,
    back,
    adj,
    csq,
    dirn,
    grad,
    gain,
    spot,
    crec,
    twice,
    recs,
    recv_mask,
    traces,
    weights,
    csq_s,
    now_s,
    prev_s,
    dirn_s,
    oldg,
    res_s,
    depth_s,
    resid_s,
    half_a,
    half_b,
    half_c,
    slots_a,
    slots_b,
    slots_c,
    local_sem,
    start_send,
    start_recv,
    halo_send,
    halo_recv,
    pair_send,
    pair_recv,
    sum_send,
    sum_recv,
    out_sem,
):
    nx, ny, nz, steps, entries = sizes
    shots, gxs, gys = groups
    parts = nz // LANES
    ex, ey = nx + 2 * DEEP, ny + 2 * TILE
    x_lo, x_hi = DEEP, DEEP + nx
    y_lo, y_hi = TILE, TILE + ny
    shot, gx, gy = lax.axis_index("shot"), lax.axis_index("gx"), lax.axis_index("gy")
    core = lax.rem(shot, 2)

    def has(way):
        at_x, at_y = gx + way[0], gy + way[1]
        return (at_x >= 0) & (at_x < gxs) & (at_y >= 0) & (at_y < gys)

    def regions(way, width):
        dx, dy = way
        src_x, dst_x = {
            -1: ((x_lo, width), (x_hi, width)),
            1: ((x_hi - width, width), (x_lo - width, width)),
            0: ((x_lo, nx), (x_lo, nx)),
        }[dx]
        src_y, dst_y = {
            -1: ((y_lo, TILE), (y_hi, TILE)),
            1: ((y_hi - TILE, TILE), (0, TILE)),
            0: ((y_lo, ny), (y_lo, ny)),
        }[dy]
        return (
            (pl.ds(*src_x), slice(None), pl.ds(*src_y), slice(None)),
            (pl.ds(*dst_x), slice(None), pl.ds(*dst_y), slice(None)),
        )

    def halo_copy(ref, k, width, send, recv):
        src, dst = regions(WAYS[k], width)
        return pltpu.make_async_remote_copy(
            src_ref=ref.at[src],
            dst_ref=ref.at[dst],
            send_sem=send.at[k],
            recv_sem=recv.at[k],
            device_id={"gx": gx + WAYS[k][0], "gy": gy + WAYS[k][1]},
            device_id_type=MESH,
        )

    def start_way(ref, k, width, send, recv):
        @pl.when(has(WAYS[k]))
        def _():
            halo_copy(ref, k, width, send, recv).start()

    def start_halo(ref, width, send, recv):
        for k in (4, 5, 6, 7, 0, 1, 2, 3):
            start_way(ref, k, width, send, recv)

    def wait_halo(ref, width, send, recv):
        for k, way in enumerate(WAYS):
            came = has((-way[0], -way[1]))

            @pl.when(came)
            def _():
                halo_copy(ref, k, width, send, recv).wait_recv()

            @pl.when(jnp.logical_not(came))
            def _():
                where = regions(way, width)[1]
                view = ref.at[where]
                view[...] = jnp.zeros(view.shape, F32)

            @pl.when(has(way))
            def _():
                halo_copy(ref, k, width, send, recv).wait_send()

    xs, ys = pl.ds(x_lo, nx), pl.ds(y_lo, ny)

    loads = [
        (res_h, res_s),
        (depth_h, depth_s),
        (csq_h, csq_s),
        (now_h, now_s),
        (prev_h, prev_s),
        (dirn_h, dirn_s),
        (oldg_h, oldg),
    ]
    copies = [
        pltpu.make_async_copy(src, dst, local_sem.at[i]) for i, (src, dst) in enumerate(loads)
    ]
    for copy in copies:
        copy.start()

    half = nx // 2
    gy_core = gys * 2
    place = gy * 2 + core
    partner = {"shot": shot + 1 - 2 * core}
    opposite = {"shot": lax.rem(shot + 2, shots)}

    def gx_member(k):
        return {"gx": k}

    def side_member(k):
        return {"gy": k // 2, "shot": shot - core + lax.rem(k, 2)}

    wide = gy * shots + shot

    def wide_member(k):
        return {"gy": k // shots, "shot": lax.rem(k, shots)}

    barrier = pltpu.get_barrier_semaphore()

    def greet(device):
        pl.semaphore_signal(barrier, inc=1, device_id=device, device_id_type=MESH)

    for o in range(1, gxs):
        greet(gx_member(lax.rem(gx + o, gxs)))
    for o in range(1, gys * shots):
        greet(wide_member(lax.rem(wide + o, gys * shots)))
    met = jnp.int32(gxs + gys * shots - 2)
    for way in WAYS[4:]:

        @pl.when(has(way))
        def _():
            greet({"gx": gx + way[0], "gy": gy + way[1]})

        met = met + has(way).astype(jnp.int32)

    lane = lax.broadcasted_iota(jnp.int32, (ey, LANES), 1)
    row = lax.broadcasted_iota(jnp.int32, (ey, LANES), 0)
    live_here = live[0]

    @pl.loop(0, ex)
    def _(i):
        for h in range(parts):
            adj[0, i, h] = jnp.zeros((ey, LANES), F32)
            hit = (row + (gy * ny - TILE) == source[0, 1]) & (lane + h * LANES == source[0, 2])
            hit = hit & (row * 0 + (i + gx * nx - DEEP) == source[0, 0])
            spot[i, h] = jnp.where(hit, 1.0, 0.0)

    recs[...] = jnp.zeros(recs.shape, F32)

    def unpack_rows(source_ref, target):
        for i in range(nx):
            for h in range(parts):
                target[i + x_lo, h, y_lo:y_hi, :] = source_ref[i, :, h * LANES : (h + 1) * LANES]

    starts = [(traces, DEEP), (csq, DEEP), (back.at[1], DEEP), (back.at[0], 1), (dirn, DEEP)]

    def start_first(i):
        start_halo(starts[i][0], starts[i][1], start_send.at[i], start_recv.at[i])

    copies[0].wait()
    copies[1].wait()
    depths = depth_s[...].astype(F32)
    top = lax.broadcasted_iota(jnp.int32, (8, ny), 0)
    for i in range(nx):
        level = jnp.where(top == 0, depths[i : i + 1], 0.0)
        rest = jnp.zeros((LANES - steps - 8, ny), F32)
        stack = jnp.concatenate([res_s[:, i, :], level, rest], axis=0)
        traces[i + x_lo, 0, y_lo:y_hi, :] = jnp.transpose(stack)
    pl.semaphore_wait(barrier, met)
    start_first(0)
    copies[2].wait()
    unpack_rows(csq_s, csq.at[...])
    start_first(1)
    copies[3].wait()
    unpack_rows(now_s, back.at[1])
    start_first(2)
    copies[4].wait()
    unpack_rows(prev_s, back.at[0])
    start_first(3)
    copies[5].wait()
    unpack_rows(dirn_s, dirn.at[...])
    copies[6].wait()

    wait_halo(traces, DEEP, start_send.at[0], start_recv.at[0])

    def column(i, n, r, count):
        at = lane[:count]
        picked = jnp.where((at == n) & (at < live_here), traces[i, 0, r : r + count, :], 0.0)
        return jnp.sum(picked, axis=1, keepdims=True)

    def receivers(i):
        level = jnp.sum(jnp.where(lane == steps, traces[i, 0], 0.0), axis=1, keepdims=True)
        return [(lane + h * LANES).astype(F32) == level for h in range(parts)]

    @pl.loop(0, ex)
    def _(i):
        for n in range(steps):
            weights[n, i] = jnp.broadcast_to(column(i, n, 0, ey), (ey, LANES))

    wait_halo(csq, DEEP, start_send.at[1], start_recv.at[1])

    @pl.loop(0, ex)
    def _(i):
        for h, here in enumerate(receivers(i)):
            crec[i, h] = jnp.where(here, csq[i, h], 0.0)
            adj[1, i, h] = crec[i, h] * weights[steps - 1, i]
            twice[i, h] = 2.0 - 6.0 * csq[i, h]

    @pl.loop(0, nx)
    def _(i):
        for h, here in enumerate(receivers(i + x_lo)):
            recv_mask[i, h] = jnp.where(here, 1.0, 0.0)[y_lo:y_hi]

    def strip(field, s, i, r, count, extra):
        at = lane[:count]
        first, last = at == 0, at == LANES - 1
        rows = pl.ds(r, count)
        mids = [field[s, i, h, rows, :] for h in range(parts)]
        ups = [pltpu.roll(mid, 1, 1) for mid in mids]
        downs = [pltpu.roll(mid, LANES - 1, 1) for mid in mids]
        for h, mid in enumerate(mids):
            before = ups[h - 1] if h > 0 else 0.0
            after = downs[h + 1] if h < parts - 1 else 0.0
            left = jnp.where(first, before, ups[h])
            right = jnp.where(last, after, downs[h])
            if r > 0:
                above = field[s, i, h, pl.ds(r - 1, count), :]
            else:
                above = pltpu.roll(mid, 1, 0)
            if r + count < ey:
                below = field[s, i, h, pl.ds(r + 1, count), :]
            else:
                below = pltpu.roll(mid, count - 1, 0)
            total = (field[s, i - 1, h, rows, :] + field[s, i + 1, h, rows, :]) + (above + below)
            total = total + (left + right)
            value = csq[i, h, rows, :] * total + twice[i, h, rows, :] * mid
            value = value - field[s - 1, i, h, rows, :] + extra(i, h, r, count)
            field[s + 1, i, h, rows, :] = value

    def plane(field, s, i, whole, extra):
        if whole:
            strip(field, s, i, 0, TILE, extra)
        strip(field, s, i, y_lo, ny, extra)
        if whole:
            strip(field, s, i, y_hi, TILE, extra)

    def planes(field, s, lo, hi, whole, extra):
        @pl.loop(lo, hi, unroll=2)
        def _(i):
            plane(field, s, i, whole, extra)

    def ahead(s):
        amount = wavelet[0, s - 1]
        return lambda i, h, r, count: amount * spot[i, h, r : r + count, :]

    def behind(s):
        n = steps - 1 - s
        return lambda i, h, r, count: crec[i, h, r : r + count, :] * weights[n, i, r : r + count, :]

    def scattered(s):
        return lambda i, h, r, count: (
            gain[i, h, r : r + count, :] * back[s + 1, i, h, r : r + count, :]
        )

    def advance(field, s, make, send, recv, width):
        first, second = make(s), make(s + 1)
        target = field.at[s + 2]
        planes(field, s, x_lo - 1, x_lo + DEEP + 1, True, first)
        planes(field, s + 1, x_lo, x_lo + DEEP, False, second)
        for k in (4, 5, 0):
            start_way(target, k, width, send, recv)
        planes(field, s, x_hi - DEEP - 1, x_hi + 1, True, first)
        planes(field, s + 1, x_hi - DEEP, x_hi, False, second)
        for k in (6, 7, 1):
            start_way(target, k, width, send, recv)
        planes(field, s, x_lo + DEEP + 1, x_hi - DEEP - 1, True, first)
        planes(field, s + 1, x_lo + DEEP, x_hi - DEEP, False, second)
        start_way(target, 2, width, send, recv)
        start_way(target, 3, width, send, recv)

    blocks = (steps - 1) // 2
    end = 2 * blocks + 1
    final = (blocks - 1) % 2
    fields = ((adj, 1, behind), (back, 0, ahead))

    def both(j, width):
        s = 2 * j + 1
        now, before = lax.rem(j, 2), lax.rem(j + 1, 2)
        for field, way, make in fields:

            @pl.when(j > 0)
            def _():
                wait_halo(field.at[s], DEEP, halo_send.at[way, before], halo_recv.at[way, before])

            if way == 0:

                @pl.when(j == 0)
                def _():
                    wait_halo(back.at[1], DEEP, start_send.at[2], start_recv.at[2])
                    wait_halo(back.at[0], 1, start_send.at[3], start_recv.at[3])

            advance(field, s, make, halo_send.at[way, now], halo_recv.at[way, now], width)

    @pl.loop(0, blocks - 1)
    def _(j):
        both(j, DEEP)

    both(jnp.int32(blocks - 1), 1)

    def product(i, h, slots):
        terms = [
            back[a, i, h, y_lo:y_hi, :] * adj[steps + 1 - a, i, h, y_lo:y_hi, :] for a in slots
        ]
        return functools.reduce(lambda one, two: one + two, terms)

    @pl.loop(x_lo, x_hi)
    def _(i):
        for h in range(parts):
            grad[i, h, y_lo:y_hi, :] = product(i, h, range(2, steps))

    for field, way, make in fields:
        wait_halo(field.at[end], 1, halo_send.at[way, final], halo_recv.at[way, final])
        planes(field, end, x_lo, x_hi, False, make(end))

    start_first(4)

    mine, other = x_lo + half * core, x_lo + half * (1 - core)

    def complete(i, h):
        return grad[i, h, y_lo:y_hi, :] + product(i, h, (1, steps))

    def pair_copy(src, dst, k, p, device):
        return pltpu.make_async_remote_copy(
            src_ref=src,
            dst_ref=dst,
            send_sem=pair_send.at[k, p],
            recv_sem=pair_recv.at[k, p],
            device_id=device,
            device_id_type=MESH,
        )

    def own_plane(p):
        return grad.at[mine + p, :, ys, :]

    def swap_a(p):
        return pair_copy(half_c.at[p], half_a.at[p], 0, p, partner)

    def swap_b(p):
        return pair_copy(own_plane(p), half_b.at[p], 1, p, opposite)

    def spread(p):
        return pair_copy(own_plane(p), own_plane(p), 2, p, partner)

    def add_plane(p, buffer):
        for h in range(parts):
            grad[mine + p, h, y_lo:y_hi, :] = grad[mine + p, h, y_lo:y_hi, :] + buffer[p, h]

    @pl.loop(0, half)
    def _(p):
        for h in range(parts):
            half_c[p, h] = complete(other + p, h)
        swap_a(p).start()

    @pl.loop(0, half)
    def _(p):
        for h in range(parts):
            grad[mine + p, h, y_lo:y_hi, :] = complete(mine + p, h)
        swap_a(p).wait()
        add_plane(p, half_a)
        swap_b(p).start()

    @pl.loop(0, half)
    def _(p):
        swap_b(p).wait()
        add_plane(p, half_b)
        spread(p).start()

    def fold(values):
        return jnp.sum(values.reshape(-1, 8, LANES), axis=0)

    def dots(i, sums):
        for h in range(parts):
            g = grad[mine + i, h, y_lo:y_hi, :]
            o = oldg[mine + i - x_lo, :, h * LANES : (h + 1) * LANES]
            d = dirn[mine + i, h, y_lo:y_hi, :]
            added = [fold(a * b) for a, b in ((g, g), (g, o), (o, o), (g, d))]
            sums = tuple(s + p for s, p in zip(sums, added))
        return sums

    zero = jnp.zeros((8, LANES), F32)
    eight = lax.broadcasted_iota(jnp.int32, (8, LANES), 0)

    def pack(sums):
        packed = zero
        for k, value in enumerate(sums):
            packed = jnp.where(eight == k, jnp.sum(value, axis=0, keepdims=True), packed)
        return packed

    def unpack(packed, k):
        return jnp.sum(packed[k : k + 1], axis=1, keepdims=True)

    sums = lax.fori_loop(0, half, dots, (zero,) * 4)
    def all_sum(values, slots, at, count, member, base):
        slots[at] = values

        def copy(peer, slot):
            return pltpu.make_async_remote_copy(
                src_ref=slots.at[at],
                dst_ref=slots.at[slot],
                send_sem=sum_send.at[base, peer],
                recv_sem=sum_recv.at[base, slot],
                device_id=member(peer),
                device_id_type=MESH,
            )

        for o in range(1, count):
            copy(lax.rem(at + o, count), at).start()
        for o in range(1, count):
            source_at = lax.rem(at + count - o, count)
            copy(source_at, source_at).wait_recv()
        for o in range(1, count):
            copy(lax.rem(at + o, count), at).wait_send()
        total = slots[0]
        for k in range(1, count):
            total = total + slots[k]
        return total

    stacked = pack(sums)
    for p in range(half):
        spread(p).wait_recv()
    start_halo(grad, DEEP, start_send.at[0], start_recv.at[0])
    stacked = all_sum(stacked, slots_a.at[0], gx, gxs, gx_member, 0)
    stacked = all_sum(stacked, slots_b, place, gy_core, side_member, 1)
    grad_sq, cross, old_sq, toward = [unpack(stacked, k) for k in range(4)]
    beta = (grad_sq - cross) / old_sq
    slope = grad_sq + beta * toward
    for p in range(half):
        spread(p).wait_send()
    wait_halo(dirn, DEEP, start_send.at[4], start_recv.at[4])
    wait_halo(grad, DEEP, start_send.at[0], start_recv.at[0])

    @pl.loop(0, ex)
    def _(i):
        for h in range(parts):
            onward = grad[i, h] + beta * dirn[i, h]
            dirn[i, h] = onward
            gain[i, h] = csq[i, h] * onward
            adj[1, i, h] = gain[i, h] * back[1, i, h]

    def sample(s):
        @pl.loop(0, nx, unroll=2)
        def _(i):
            seen = adj[s, i + x_lo, 0, y_lo:y_hi, :] * recv_mask[i, 0]
            for h in range(1, parts):
                seen = seen + adj[s, i + x_lo, h, y_lo:y_hi, :] * recv_mask[i, h]
            value = jnp.sum(seen, axis=1, keepdims=True)
            recs[i] = jnp.where(lane[:ny] == s - 1, value, recs[i])

    @pl.loop(0, nx)
    def _(i):
        for h in range(parts):
            dirn_s[i, :, h * LANES : (h + 1) * LANES] = grad[i + x_lo, h, y_lo:y_hi, :]

    out_grad = pltpu.make_async_copy(dirn_s, grad_h, out_sem.at[0])
    out_grad.start()
    sample(1)

    def born(j, width):
        s = 2 * j + 1
        now, before = lax.rem(j, 2), lax.rem(j + 1, 2)

        @pl.when(j > 0)
        def _():
            wait_halo(adj.at[s], DEEP, halo_send.at[2, before], halo_recv.at[2, before])

        advance(adj, s, scattered, halo_send.at[2, now], halo_recv.at[2, now], width)
        sample(s + 1)
        sample(s + 2)

    @pl.loop(0, blocks - 1)
    def _(j):
        born(j, DEEP)

    born(jnp.int32(blocks - 1), 1)
    wait_halo(adj.at[end], 1, halo_send.at[2, final], halo_recv.at[2, final])
    planes(adj, end, x_lo, x_hi, False, scattered(end))
    sample(end + 1)

    lane_r = lane[:ny]
    told = lane_r < live_here
    kept = lane_r < steps

    def score(i, sums):
        rec = jnp.where(told, recs[i], 0.0)
        res = jnp.where(kept, traces[i + x_lo, 0, y_lo:y_hi, :], 0.0)
        recs[i] = rec
        added = [fold(a * b) for a, b in ((rec, rec), (rec, res), (res, res))]
        return tuple(s + p for s, p in zip(sums, added))

    sums = lax.fori_loop(0, nx, score, (zero,) * 3)
    for i in range(nx):
        resid_s[:, i, :] = jnp.transpose(recs[i])[:steps]

    out_born = pltpu.make_async_copy(resid_s, born_h, out_sem.at[1])
    out_born.start()
    stacked = pack(sums)
    stacked = all_sum(stacked, slots_a.at[1], gx, gxs, gx_member, 2)
    stacked = all_sum(stacked, slots_c, wide, gys * shots, wide_member, 3)
    rec_sq, rec_res, res_sq = [unpack(stacked, k) for k in range(3)]
    length = slope / rec_sq

    misfit = res_sq - 2.0 * length * rec_res + length * length * rec_sq
    scalars = jnp.where(eight == 0, beta, jnp.where(eight == 1, length, misfit * (0.5 / entries)))
    scalars_o[...] = scalars
    out_grad.wait()
    out_born.wait()


def finish(scalars, grad, dirn, refl, residual, born, image, onward, resid, misfit):
    beta, length = scalars[0:1, 0:1], scalars[1:2, 0:1]
    misfit[0, 0] = jnp.sum(scalars[2:3, 0:1])

    @pl.loop(0, grad.shape[0])
    def _(i):
        path = grad[i] + beta * dirn[i]
        onward[i] = path
        image[i] = refl[i] + length * path

    @pl.loop(0, residual.shape[0])
    def _(n):
        resid[n] = residual[n] - length * born[n]


def on_device(groups, *arguments):
    (now, prev, csq, refl, dirn, oldg, residual, depth, source, wavelet, live) = arguments
    now, prev = now[0], prev[0]
    nx, ny, nz = now.shape
    steps = residual.shape[1]
    entries = float(residual.size * groups[0] * groups[1] * groups[2])
    ex, ey = nx + 2 * DEEP, ny + 2 * TILE
    whole = pl.BlockSpec(memory_space=pl.ANY)
    small = pl.BlockSpec(memory_space=pltpu.SMEM)
    parts = nz // LANES
    grow = pltpu.VMEM((ex, parts, ey, LANES), F32)
    block = pltpu.VMEM((nx, parts, ny, LANES), F32)
    stage = pltpu.VMEM((nx, ny, nz), F32)
    piece = pltpu.VMEM((nx // 2, parts, ny, LANES), F32)
    history = pltpu.VMEM((steps + 1, ex, parts, ey, LANES), F32)
    dma = pltpu.SemaphoreType.DMA
    grad, born, scalars = pl.pallas_call(
        functools.partial(kernel, (nx, ny, nz, steps, entries), groups),
        out_shape=(
            jax.ShapeDtypeStruct((nx, ny, nz), F32),
            jax.ShapeDtypeStruct((steps, nx, ny), F32),
            jax.ShapeDtypeStruct((8, 128), F32),
        ),
        in_specs=[whole] * 7 + [small] * 3,
        out_specs=(whole, whole, pl.BlockSpec(memory_space=pltpu.VMEM)),
        scratch_shapes=[
            history,
            history,
            grow,
            grow,
            grow,
            grow,
            grow,
            grow,
            grow,
            pltpu.VMEM((nx, ny, LANES), F32),
            block,
            pltpu.VMEM((ex, 1, ey, LANES), F32),
            pltpu.VMEM((steps, ex, ey, LANES), F32),
            stage,
            stage,
            stage,
            stage,
            stage,
            pltpu.VMEM((steps, nx, ny), F32),
            pltpu.VMEM((nx, ny), jnp.int32),
            pltpu.VMEM((steps, nx, ny), F32),
            piece,
            piece,
            piece,
            pltpu.VMEM((2, groups[1], 8, LANES), F32),
            pltpu.VMEM((groups[2] * 2, 8, LANES), F32),
            pltpu.VMEM((groups[2] * groups[0], 8, LANES), F32),
            dma((7,)),
            dma((5, 8)),
            dma((5, 8)),
            dma((3, 2, 8)),
            dma((3, 2, 8)),
            dma((3, nx // 2)),
            dma((3, nx // 2)),
            dma((4, 16)),
            dma((4, 16)),
            dma((2,)),
        ],
        compiler_params=pltpu.CompilerParams(
            has_side_effects=True, collective_id=0, vmem_limit_bytes=62 * 1024 * 1024
        ),
        name="iteration",
    )(now, prev, csq, dirn, oldg, residual[0], depth[0], source, wavelet, live)
    vector = pl.BlockSpec(memory_space=pltpu.VMEM)
    image, onward, resid, misfit = pl.pallas_call(
        finish,
        out_shape=(
            jax.ShapeDtypeStruct((nx, ny, nz), F32),
            jax.ShapeDtypeStruct((nx, ny, nz), F32),
            jax.ShapeDtypeStruct((steps, nx, ny), F32),
            jax.ShapeDtypeStruct((1, 1), F32),
        ),
        in_specs=[vector] * 6,
        out_specs=(vector, vector, vector, small),
        name="finish",
    )(scalars, grad, dirn, refl, residual[0], born)
    return image, onward, resid[None], misfit[0, 0]


def solution(mesh):
    groups = (mesh.shape["shot"], mesh.shape["gx"], mesh.shape["gy"])
    space = P("gx", "gy", None)
    placed = (
        P("shot", "gx", "gy", None),
        P("shot", "gx", "gy", None),
        space,
        space,
        space,
        space,
        P("shot", None, "gx", "gy"),
        P("shot", "gx", "gy"),
        P("shot", None),
        P("shot", None),
        P("shot"),
    )
    return jax.shard_map(
        functools.partial(on_device, groups),
        mesh=mesh,
        in_specs=placed,
        out_specs=(space, space, P("shot", None, "gx", "gy"), P()),
        check_vma=False,
    )
```

```python
import functools

import jax
import jax.numpy as jnp
from jax import lax
from jax.experimental import pallas as pl
from jax.experimental.pallas import tpu as pltpu
from jax.sharding import PartitionSpec as P

MESH = pl.DeviceIdType.MESH
F32 = jnp.float32
WAYS = [(-1, 0), (1, 0), (0, -1), (0, 1), (-1, -1), (-1, 1), (1, -1), (1, 1)]
DEEP = 2
TILE = 8
LANES = 128


def kernel(
    sizes,
    groups,
    now_h,
    prev_h,
    csq_h,
    dirn_h,
    oldg_h,
    res_h,
    depth_h,
    source,
    wavelet,
    live,
    grad_h,
    born_h,
    scalars_o,
    back,
    adj,
    csq,
    dirn,
    grad,
    gain,
    spot,
    crec,
    twice,
    recs,
    recv_mask,
    traces,
    weights,
    csq_s,
    now_s,
    prev_s,
    dirn_s,
    oldg,
    res_s,
    depth_s,
    resid_s,
    half_a,
    half_b,
    half_c,
    slots_a,
    slots_b,
    slots_c,
    local_sem,
    start_send,
    start_recv,
    halo_send,
    halo_recv,
    pair_send,
    pair_recv,
    sum_send,
    sum_recv,
    out_sem,
):
    nx, ny, nz, steps, entries = sizes
    shots, gxs, gys = groups
    parts = nz // LANES
    ex, ey = nx + 2 * DEEP, ny + 2 * TILE
    x_lo, x_hi = DEEP, DEEP + nx
    y_lo, y_hi = TILE, TILE + ny
    shot, gx, gy = lax.axis_index("shot"), lax.axis_index("gx"), lax.axis_index("gy")
    core = lax.rem(shot, 2)

    def has(way):
        at_x, at_y = gx + way[0], gy + way[1]
        return (at_x >= 0) & (at_x < gxs) & (at_y >= 0) & (at_y < gys)

    def regions(way, width):
        dx, dy = way
        src_x, dst_x = {
            -1: ((x_lo, width), (x_hi, width)),
            1: ((x_hi - width, width), (x_lo - width, width)),
            0: ((x_lo, nx), (x_lo, nx)),
        }[dx]
        src_y, dst_y = {
            -1: ((y_lo, TILE), (y_hi, TILE)),
            1: ((y_hi - TILE, TILE), (0, TILE)),
            0: ((y_lo, ny), (y_lo, ny)),
        }[dy]
        return (
            (pl.ds(*src_x), slice(None), pl.ds(*src_y), slice(None)),
            (pl.ds(*dst_x), slice(None), pl.ds(*dst_y), slice(None)),
        )

    def depth_of(k, width):
        return width if k < 4 else 1

    def halo_copy(ref, k, width, send, recv):
        src, dst = regions(WAYS[k], depth_of(k, width))
        return pltpu.make_async_remote_copy(
            src_ref=ref.at[src],
            dst_ref=ref.at[dst],
            send_sem=send.at[k],
            recv_sem=recv.at[k],
            device_id={"gx": gx + WAYS[k][0], "gy": gy + WAYS[k][1]},
            device_id_type=MESH,
        )

    def start_way(ref, k, width, send, recv):
        @pl.when(has(WAYS[k]))
        def _():
            halo_copy(ref, k, width, send, recv).start()

    def used(width):
        return (4, 5, 6, 7, 0, 1, 2, 3) if width == DEEP else (0, 1, 2, 3)

    def start_halo(ref, width, send, recv):
        for k in used(width):
            start_way(ref, k, width, send, recv)

    def wait_halo(ref, width, send, recv):
        for k in used(width):
            way = WAYS[k]
            came = has((-way[0], -way[1]))

            @pl.when(came)
            def _():
                halo_copy(ref, k, width, send, recv).wait_recv()

            @pl.when(jnp.logical_not(came))
            def _():
                where = regions(way, depth_of(k, width))[1]
                view = ref.at[where]
                view[...] = jnp.zeros(view.shape, F32)

            @pl.when(has(way))
            def _():
                halo_copy(ref, k, width, send, recv).wait_send()

    xs, ys = pl.ds(x_lo, nx), pl.ds(y_lo, ny)

    loads = [
        (res_h, res_s),
        (depth_h, depth_s),
        (csq_h, csq_s),
        (now_h, now_s),
        (prev_h, prev_s),
        (dirn_h, dirn_s),
        (oldg_h, oldg),
    ]
    copies = [
        pltpu.make_async_copy(src, dst, local_sem.at[i]) for i, (src, dst) in enumerate(loads)
    ]
    for copy in copies:
        copy.start()

    half = nx // 2
    gy_core = gys * 2
    place = gy * 2 + core
    partner = {"shot": shot + 1 - 2 * core}
    opposite = {"shot": lax.rem(shot + 2, shots)}

    def gx_member(k):
        return {"gx": k}

    def side_member(k):
        return {"gy": k // 2, "shot": shot - core + lax.rem(k, 2)}

    wide = gy * shots + shot

    def wide_member(k):
        return {"gy": k // shots, "shot": lax.rem(k, shots)}

    barrier = pltpu.get_barrier_semaphore()

    def greet(device):
        pl.semaphore_signal(barrier, inc=1, device_id=device, device_id_type=MESH)

    for o in range(1, gxs):
        greet(gx_member(lax.rem(gx + o, gxs)))
    for o in range(1, gys * shots):
        greet(wide_member(lax.rem(wide + o, gys * shots)))
    met = jnp.int32(gxs + gys * shots - 2)
    for way in WAYS[4:]:

        @pl.when(has(way))
        def _():
            greet({"gx": gx + way[0], "gy": gy + way[1]})

        met = met + has(way).astype(jnp.int32)

    lane = lax.broadcasted_iota(jnp.int32, (ey, LANES), 1)
    row = lax.broadcasted_iota(jnp.int32, (ey, LANES), 0)
    live_here = live[0]

    @pl.loop(0, ex)
    def _(i):
        for h in range(parts):
            adj[0, i, h] = jnp.zeros((ey, LANES), F32)
            hit = (row + (gy * ny - TILE) == source[0, 1]) & (lane + h * LANES == source[0, 2])
            hit = hit & (row * 0 + (i + gx * nx - DEEP) == source[0, 0])
            spot[i, h] = jnp.where(hit, 1.0, 0.0)

    recs[...] = jnp.zeros(recs.shape, F32)

    def unpack_rows(source_ref, target):
        for i in range(nx):
            for h in range(parts):
                target[i + x_lo, h, y_lo:y_hi, :] = source_ref[i, :, h * LANES : (h + 1) * LANES]

    starts = [(traces, DEEP), (csq, DEEP), (back.at[1], DEEP), (back.at[0], 1), (dirn, DEEP)]

    def start_first(i):
        start_halo(starts[i][0], starts[i][1], start_send.at[i], start_recv.at[i])

    copies[0].wait()
    copies[1].wait()
    depths = depth_s[...].astype(F32)
    top = lax.broadcasted_iota(jnp.int32, (8, ny), 0)
    for i in range(nx):
        level = jnp.where(top == 0, depths[i : i + 1], 0.0)
        rest = jnp.zeros((LANES - steps - 8, ny), F32)
        stack = jnp.concatenate([res_s[:, i, :], level, rest], axis=0)
        traces[i + x_lo, 0, y_lo:y_hi, :] = jnp.transpose(stack)
    pl.semaphore_wait(barrier, met)
    start_first(0)
    copies[2].wait()
    unpack_rows(csq_s, csq.at[...])
    start_first(1)
    copies[3].wait()
    unpack_rows(now_s, back.at[1])
    start_first(2)
    copies[4].wait()
    unpack_rows(prev_s, back.at[0])
    start_first(3)
    copies[5].wait()
    unpack_rows(dirn_s, dirn.at[...])
    copies[6].wait()

    wait_halo(traces, DEEP, start_send.at[0], start_recv.at[0])

    def column(i, n, r, count):
        at = lane[:count]
        picked = jnp.where((at == n) & (at < live_here), traces[i, 0, r : r + count, :], 0.0)
        return jnp.sum(picked, axis=1, keepdims=True)

    def receivers(i):
        level = jnp.sum(jnp.where(lane == steps, traces[i, 0], 0.0), axis=1, keepdims=True)
        return [(lane + h * LANES).astype(F32) == level for h in range(parts)]

    @pl.loop(0, ex)
    def _(i):
        for n in range(steps):
            weights[n, i] = jnp.broadcast_to(column(i, n, 0, ey), (ey, LANES))

    wait_halo(csq, DEEP, start_send.at[1], start_recv.at[1])

    @pl.loop(0, ex)
    def _(i):
        for h, here in enumerate(receivers(i)):
            crec[i, h] = jnp.where(here, csq[i, h], 0.0)
            adj[1, i, h] = crec[i, h] * weights[steps - 1, i]
            twice[i, h] = 2.0 - 6.0 * csq[i, h]

    @pl.loop(0, nx)
    def _(i):
        for h, here in enumerate(receivers(i + x_lo)):
            recv_mask[i, h] = jnp.where(here, 1.0, 0.0)[y_lo:y_hi]

    def strip(field, s, i, r, count, extra):
        at = lane[:count]
        first, last = at == 0, at == LANES - 1
        rows = pl.ds(r, count)
        mids = [field[s, i, h, rows, :] for h in range(parts)]
        ups = [pltpu.roll(mid, 1, 1) for mid in mids]
        downs = [pltpu.roll(mid, LANES - 1, 1) for mid in mids]
        for h, mid in enumerate(mids):
            before = ups[h - 1] if h > 0 else 0.0
            after = downs[h + 1] if h < parts - 1 else 0.0
            left = jnp.where(first, before, ups[h])
            right = jnp.where(last, after, downs[h])
            if r > 0:
                above = field[s, i, h, pl.ds(r - 1, count), :]
            else:
                above = pltpu.roll(mid, 1, 0)
            if r + count < ey:
                below = field[s, i, h, pl.ds(r + 1, count), :]
            else:
                below = pltpu.roll(mid, count - 1, 0)
            total = (field[s, i - 1, h, rows, :] + field[s, i + 1, h, rows, :]) + (above + below)
            total = total + (left + right)
            value = csq[i, h, rows, :] * total + twice[i, h, rows, :] * mid
            value = value - field[s - 1, i, h, rows, :] + extra(i, h, r, count)
            field[s + 1, i, h, rows, :] = value

    def plane(field, s, i, whole, extra):
        if whole:
            strip(field, s, i, 0, TILE, extra)
        strip(field, s, i, y_lo, ny, extra)
        if whole:
            strip(field, s, i, y_hi, TILE, extra)

    def planes(field, s, lo, hi, whole, extra):
        @pl.loop(lo, hi, unroll=3 if (hi - lo) % 2 else 2)
        def _(i):
            plane(field, s, i, whole, extra)

    def ahead(s):
        amount = wavelet[0, s - 1]
        return lambda i, h, r, count: amount * spot[i, h, r : r + count, :]

    def behind(s):
        n = steps - 1 - s
        return lambda i, h, r, count: crec[i, h, r : r + count, :] * weights[n, i, r : r + count, :]

    def scattered(s):
        return lambda i, h, r, count: (
            gain[i, h, r : r + count, :] * back[s + 1, i, h, r : r + count, :]
        )

    def advance(field, s, make, send, recv, width):
        first, second = make(s), make(s + 1)
        target = field.at[s + 2]
        left, right = x_lo, x_hi - 1

        def go(*ways):
            for k in ways:
                if k in used(width):
                    start_way(target, k, width, send, recv)

        planes(field, s, left - 1, left + 2, True, first)
        plane(field, s + 1, left, False, second)
        go(4, 5)
        planes(field, s, right - 1, right + 2, True, first)
        plane(field, s + 1, right, False, second)
        go(6, 7)
        plane(field, s, left + 2, True, first)
        plane(field, s + 1, left + 1, False, second)
        go(0)
        plane(field, s, right - 2, True, first)
        plane(field, s + 1, right - 1, False, second)
        go(1)
        planes(field, s, left + 3, right - 2, True, first)
        planes(field, s + 1, left + 2, right - 1, False, second)
        go(2, 3)

    blocks = (steps - 1) // 2
    end = 2 * blocks + 1
    final = (blocks - 1) % 2
    fields = ((adj, 1, behind), (back, 0, ahead))

    def both(j, width):
        s = 2 * j + 1
        now, before = lax.rem(j, 2), lax.rem(j + 1, 2)
        for field, way, make in fields:

            @pl.when(j > 0)
            def _():
                wait_halo(field.at[s], DEEP, halo_send.at[way, before], halo_recv.at[way, before])

            if way == 0:

                @pl.when(j == 0)
                def _():
                    wait_halo(back.at[1], DEEP, start_send.at[2], start_recv.at[2])
                    wait_halo(back.at[0], 1, start_send.at[3], start_recv.at[3])

            advance(field, s, make, halo_send.at[way, now], halo_recv.at[way, now], width)

    @pl.loop(0, blocks - 1)
    def _(j):
        both(j, DEEP)

    both(jnp.int32(blocks - 1), 1)

    def product(i, h, slots):
        terms = [
            back[a, i, h, y_lo:y_hi, :] * adj[steps + 1 - a, i, h, y_lo:y_hi, :] for a in slots
        ]
        return functools.reduce(lambda one, two: one + two, terms)

    @pl.loop(x_lo, x_hi)
    def _(i):
        for h in range(parts):
            grad[i, h, y_lo:y_hi, :] = product(i, h, range(2, steps))

    for field, way, make in fields:
        wait_halo(field.at[end], 1, halo_send.at[way, final], halo_recv.at[way, final])
        planes(field, end, x_lo, x_hi, False, make(end))

    start_first(4)

    mine, other = x_lo + half * core, x_lo + half * (1 - core)

    def complete(i, h):
        return grad[i, h, y_lo:y_hi, :] + product(i, h, (1, steps))

    def pair_copy(src, dst, k, p, device):
        return pltpu.make_async_remote_copy(
            src_ref=src,
            dst_ref=dst,
            send_sem=pair_send.at[k, p],
            recv_sem=pair_recv.at[k, p],
            device_id=device,
            device_id_type=MESH,
        )

    def own_plane(p):
        return grad.at[mine + p, :, ys, :]

    def swap_a(p):
        return pair_copy(half_c.at[p], half_a.at[p], 0, p, partner)

    def swap_b(p):
        return pair_copy(own_plane(p), half_b.at[p], 1, p, opposite)

    def spread(p):
        return pair_copy(own_plane(p), own_plane(p), 2, p, partner)

    def add_plane(p, buffer):
        for h in range(parts):
            grad[mine + p, h, y_lo:y_hi, :] = grad[mine + p, h, y_lo:y_hi, :] + buffer[p, h]

    @pl.loop(0, half)
    def _(p):
        for h in range(parts):
            half_c[p, h] = complete(other + p, h)
        swap_a(p).start()

    @pl.loop(0, half)
    def _(p):
        for h in range(parts):
            grad[mine + p, h, y_lo:y_hi, :] = complete(mine + p, h)
        swap_a(p).wait()
        add_plane(p, half_a)
        swap_b(p).start()

    @pl.loop(0, half)
    def _(p):
        swap_b(p).wait()
        add_plane(p, half_b)
        spread(p).start()

    def fold(values):
        return jnp.sum(values.reshape(-1, 8, LANES), axis=0)

    def dots(i, sums):
        for h in range(parts):
            g = grad[mine + i, h, y_lo:y_hi, :]
            o = oldg[mine + i - x_lo, :, h * LANES : (h + 1) * LANES]
            d = dirn[mine + i, h, y_lo:y_hi, :]
            added = [fold(a * b) for a, b in ((g, g), (g, o), (o, o), (g, d))]
            sums = tuple(s + p for s, p in zip(sums, added))
        return sums

    zero = jnp.zeros((8, LANES), F32)
    eight = lax.broadcasted_iota(jnp.int32, (8, LANES), 0)

    def pack(sums):
        packed = zero
        for k, value in enumerate(sums):
            packed = jnp.where(eight == k, jnp.sum(value, axis=0, keepdims=True), packed)
        return packed

    def unpack(packed, k):
        return jnp.sum(packed[k : k + 1], axis=1, keepdims=True)

    sums = lax.fori_loop(0, half, dots, (zero,) * 4)
    def all_sum(values, slots, at, count, member, base):
        slots[at] = values

        def copy(peer, slot):
            return pltpu.make_async_remote_copy(
                src_ref=slots.at[at],
                dst_ref=slots.at[slot],
                send_sem=sum_send.at[base, peer],
                recv_sem=sum_recv.at[base, slot],
                device_id=member(peer),
                device_id_type=MESH,
            )

        for o in range(1, count):
            copy(lax.rem(at + o, count), at).start()
        for o in range(1, count):
            source_at = lax.rem(at + count - o, count)
            copy(source_at, source_at).wait_recv()
        for o in range(1, count):
            copy(lax.rem(at + o, count), at).wait_send()
        total = slots[0]
        for k in range(1, count):
            total = total + slots[k]
        return total

    stacked = pack(sums)
    for p in range(half):
        spread(p).wait_recv()
    start_halo(grad, DEEP, start_send.at[0], start_recv.at[0])
    stacked = all_sum(stacked, slots_a.at[0], gx, gxs, gx_member, 0)
    stacked = all_sum(stacked, slots_b, place, gy_core, side_member, 1)
    grad_sq, cross, old_sq, toward = [unpack(stacked, k) for k in range(4)]
    beta = (grad_sq - cross) / old_sq
    slope = grad_sq + beta * toward
    for p in range(half):
        spread(p).wait_send()
    wait_halo(dirn, DEEP, start_send.at[4], start_recv.at[4])
    wait_halo(grad, DEEP, start_send.at[0], start_recv.at[0])

    @pl.loop(0, ex)
    def _(i):
        for h in range(parts):
            onward = grad[i, h] + beta * dirn[i, h]
            dirn[i, h] = onward
            gain[i, h] = csq[i, h] * onward
            adj[1, i, h] = gain[i, h] * back[1, i, h]

    def sample(s):
        @pl.loop(0, nx, unroll=2)
        def _(i):
            seen = adj[s, i + x_lo, 0, y_lo:y_hi, :] * recv_mask[i, 0]
            for h in range(1, parts):
                seen = seen + adj[s, i + x_lo, h, y_lo:y_hi, :] * recv_mask[i, h]
            value = jnp.sum(seen, axis=1, keepdims=True)
            recs[i] = jnp.where(lane[:ny] == s - 1, value, recs[i])

    @pl.loop(0, nx)
    def _(i):
        for h in range(parts):
            dirn_s[i, :, h * LANES : (h + 1) * LANES] = grad[i + x_lo, h, y_lo:y_hi, :]

    out_grad = pltpu.make_async_copy(dirn_s, grad_h, out_sem.at[0])
    out_grad.start()
    sample(1)

    def born(j, width):
        s = 2 * j + 1
        now, before = lax.rem(j, 2), lax.rem(j + 1, 2)

        @pl.when(j > 0)
        def _():
            wait_halo(adj.at[s], DEEP, halo_send.at[2, before], halo_recv.at[2, before])

        advance(adj, s, scattered, halo_send.at[2, now], halo_recv.at[2, now], width)
        sample(s + 1)
        sample(s + 2)

    @pl.loop(0, blocks - 1)
    def _(j):
        born(j, DEEP)

    born(jnp.int32(blocks - 1), 1)
    wait_halo(adj.at[end], 1, halo_send.at[2, final], halo_recv.at[2, final])
    planes(adj, end, x_lo, x_hi, False, scattered(end))
    sample(end + 1)

    lane_r = lane[:ny]
    told = lane_r < live_here
    kept = lane_r < steps

    def score(i, sums):
        rec = jnp.where(told, recs[i], 0.0)
        res = jnp.where(kept, traces[i + x_lo, 0, y_lo:y_hi, :], 0.0)
        recs[i] = rec
        added = [fold(a * b) for a, b in ((rec, rec), (rec, res), (res, res))]
        return tuple(s + p for s, p in zip(sums, added))

    sums = lax.fori_loop(0, nx, score, (zero,) * 3)
    for i in range(nx):
        resid_s[:, i, :] = jnp.transpose(recs[i])[:steps]

    out_born = pltpu.make_async_copy(resid_s, born_h, out_sem.at[1])
    out_born.start()
    stacked = pack(sums)
    stacked = all_sum(stacked, slots_a.at[1], gx, gxs, gx_member, 2)
    stacked = all_sum(stacked, slots_c, wide, gys * shots, wide_member, 3)
    rec_sq, rec_res, res_sq = [unpack(stacked, k) for k in range(3)]
    length = slope / rec_sq

    misfit = res_sq - 2.0 * length * rec_res + length * length * rec_sq
    scalars = jnp.where(eight == 0, beta, jnp.where(eight == 1, length, misfit * (0.5 / entries)))
    scalars_o[...] = scalars
    out_grad.wait()
    out_born.wait()


def finish(scalars, grad, dirn, refl, residual, born, image, onward, resid, misfit):
    beta, length = scalars[0:1, 0:1], scalars[1:2, 0:1]
    misfit[0, 0] = jnp.sum(scalars[2:3, 0:1])

    @pl.loop(0, grad.shape[0])
    def _(i):
        path = grad[i] + beta * dirn[i]
        onward[i] = path
        image[i] = refl[i] + length * path

    @pl.loop(0, residual.shape[0])
    def _(n):
        resid[n] = residual[n] - length * born[n]


def on_device(groups, *arguments):
    (now, prev, csq, refl, dirn, oldg, residual, depth, source, wavelet, live) = arguments
    now, prev = now[0], prev[0]
    nx, ny, nz = now.shape
    steps = residual.shape[1]
    entries = float(residual.size * groups[0] * groups[1] * groups[2])
    ex, ey = nx + 2 * DEEP, ny + 2 * TILE
    whole = pl.BlockSpec(memory_space=pl.ANY)
    small = pl.BlockSpec(memory_space=pltpu.SMEM)
    parts = nz // LANES
    grow = pltpu.VMEM((ex, parts, ey, LANES), F32)
    block = pltpu.VMEM((nx, parts, ny, LANES), F32)
    stage = pltpu.VMEM((nx, ny, nz), F32)
    piece = pltpu.VMEM((nx // 2, parts, ny, LANES), F32)
    history = pltpu.VMEM((steps + 1, ex, parts, ey, LANES), F32)
    dma = pltpu.SemaphoreType.DMA
    grad, born, scalars = pl.pallas_call(
        functools.partial(kernel, (nx, ny, nz, steps, entries), groups),
        out_shape=(
            jax.ShapeDtypeStruct((nx, ny, nz), F32),
            jax.ShapeDtypeStruct((steps, nx, ny), F32),
            jax.ShapeDtypeStruct((8, 128), F32),
        ),
        in_specs=[whole] * 7 + [small] * 3,
        out_specs=(whole, whole, pl.BlockSpec(memory_space=pltpu.VMEM)),
        scratch_shapes=[
            history,
            history,
            grow,
            grow,
            grow,
            grow,
            grow,
            grow,
            grow,
            pltpu.VMEM((nx, ny, LANES), F32),
            block,
            pltpu.VMEM((ex, 1, ey, LANES), F32),
            pltpu.VMEM((steps, ex, ey, LANES), F32),
            stage,
            stage,
            stage,
            stage,
            stage,
            pltpu.VMEM((steps, nx, ny), F32),
            pltpu.VMEM((nx, ny), jnp.int32),
            pltpu.VMEM((steps, nx, ny), F32),
            piece,
            piece,
            piece,
            pltpu.VMEM((2, groups[1], 8, LANES), F32),
            pltpu.VMEM((groups[2] * 2, 8, LANES), F32),
            pltpu.VMEM((groups[2] * groups[0], 8, LANES), F32),
            dma((7,)),
            dma((5, 8)),
            dma((5, 8)),
            dma((3, 2, 8)),
            dma((3, 2, 8)),
            dma((3, nx // 2)),
            dma((3, nx // 2)),
            dma((4, 16)),
            dma((4, 16)),
            dma((2,)),
        ],
        compiler_params=pltpu.CompilerParams(
            has_side_effects=True, collective_id=0, vmem_limit_bytes=62 * 1024 * 1024
        ),
        name="iteration",
    )(now, prev, csq, dirn, oldg, residual[0], depth[0], source, wavelet, live)
    vector = pl.BlockSpec(memory_space=pltpu.VMEM)
    image, onward, resid, misfit = pl.pallas_call(
        finish,
        out_shape=(
            jax.ShapeDtypeStruct((nx, ny, nz), F32),
            jax.ShapeDtypeStruct((nx, ny, nz), F32),
            jax.ShapeDtypeStruct((steps, nx, ny), F32),
            jax.ShapeDtypeStruct((1, 1), F32),
        ),
        in_specs=[vector] * 6,
        out_specs=(vector, vector, vector, small),
        name="finish",
    )(scalars, grad, dirn, refl, residual[0], born)
    return image, onward, resid[None], misfit[0, 0]


def solution(mesh):
    groups = (mesh.shape["shot"], mesh.shape["gx"], mesh.shape["gy"])
    space = P("gx", "gy", None)
    placed = (
        P("shot", "gx", "gy", None),
        P("shot", "gx", "gy", None),
        space,
        space,
        space,
        space,
        P("shot", None, "gx", "gy"),
        P("shot", "gx", "gy"),
        P("shot", None),
        P("shot", None),
        P("shot"),
    )
    return jax.shard_map(
        functools.partial(on_device, groups),
        mesh=mesh,
        in_specs=placed,
        out_specs=(space, space, P("shot", None, "gx", "gy"), P()),
        check_vma=False,
    )
```

```python
import functools

import jax
import jax.numpy as jnp
from jax import lax
from jax.experimental import pallas as pl
from jax.experimental.pallas import tpu as pltpu
from jax.sharding import PartitionSpec as P

MESH = pl.DeviceIdType.MESH
F32 = jnp.float32
WAYS = [(-1, 0), (1, 0), (0, -1), (0, 1), (-1, -1), (-1, 1), (1, -1), (1, 1)]
DEEP = 2
TILE = 8
LANES = 128


def kernel(
    sizes,
    groups,
    now_h,
    prev_h,
    csq_h,
    dirn_h,
    oldg_h,
    res_h,
    depth_h,
    source,
    wavelet,
    live,
    grad_h,
    born_h,
    scalars_o,
    back,
    adj,
    csq,
    dirn,
    grad,
    gain,
    spot,
    crec,
    twice,
    recs,
    recv_mask,
    traces,
    weights,
    csq_s,
    now_s,
    prev_s,
    dirn_s,
    oldg,
    res_s,
    depth_s,
    resid_s,
    half_a,
    half_b,
    half_c,
    slots_a,
    slots_b,
    slots_c,
    local_sem,
    start_send,
    start_recv,
    halo_send,
    halo_recv,
    pair_send,
    pair_recv,
    sum_send,
    sum_recv,
    out_sem,
):
    nx, ny, nz, steps, entries = sizes
    shots, gxs, gys = groups
    parts = nz // LANES
    ex, ey = nx + 2 * DEEP, ny + 2 * TILE
    x_lo, x_hi = DEEP, DEEP + nx
    y_lo, y_hi = TILE, TILE + ny
    shot, gx, gy = lax.axis_index("shot"), lax.axis_index("gx"), lax.axis_index("gy")
    core = lax.rem(shot, 2)

    def has(way):
        at_x, at_y = gx + way[0], gy + way[1]
        return (at_x >= 0) & (at_x < gxs) & (at_y >= 0) & (at_y < gys)

    def regions(way, width):
        dx, dy = way
        src_x, dst_x = {
            -1: ((x_lo, width), (x_hi, width)),
            1: ((x_hi - width, width), (x_lo - width, width)),
            0: ((x_lo, nx), (x_lo, nx)),
        }[dx]
        src_y, dst_y = {
            -1: ((y_lo, TILE), (y_hi, TILE)),
            1: ((y_hi - TILE, TILE), (0, TILE)),
            0: ((y_lo, ny), (y_lo, ny)),
        }[dy]
        return (
            (pl.ds(*src_x), slice(None), pl.ds(*src_y), slice(None)),
            (pl.ds(*dst_x), slice(None), pl.ds(*dst_y), slice(None)),
        )

    def depth_of(k, width):
        return width if k < 4 else 1

    def halo_copy(ref, k, width, send, recv):
        src, dst = regions(WAYS[k], depth_of(k, width))
        return pltpu.make_async_remote_copy(
            src_ref=ref.at[src],
            dst_ref=ref.at[dst],
            send_sem=send.at[k],
            recv_sem=recv.at[k],
            device_id={"gx": gx + WAYS[k][0], "gy": gy + WAYS[k][1]},
            device_id_type=MESH,
        )

    def start_way(ref, k, width, send, recv):
        @pl.when(has(WAYS[k]))
        def _():
            halo_copy(ref, k, width, send, recv).start()

    def used(width):
        return (4, 5, 6, 7, 0, 1, 2, 3) if width == DEEP else (0, 1, 2, 3)

    def start_halo(ref, width, send, recv):
        for k in used(width):
            start_way(ref, k, width, send, recv)

    def wait_halo(ref, width, send, recv, ways=range(8)):
        for k in [k for k in used(width) if k in ways]:
            way = WAYS[k]
            came = has((-way[0], -way[1]))

            @pl.when(came)
            def _():
                halo_copy(ref, k, width, send, recv).wait_recv()

            @pl.when(jnp.logical_not(came))
            def _():
                where = regions(way, depth_of(k, width))[1]
                view = ref.at[where]
                view[...] = jnp.zeros(view.shape, F32)

            @pl.when(has(way))
            def _():
                halo_copy(ref, k, width, send, recv).wait_send()

    def side_copy(ref, t, dy, width, send, recv):
        src_y, dst_y = {
            -1: ((y_lo, TILE), (y_hi, TILE)),
            1: ((y_hi - TILE, TILE), (0, TILE)),
            0: ((y_lo, ny), (y_lo, ny)),
        }[dy]
        deep = width if dy == 0 else 1
        k = t if dy == 0 else 4 + 2 * t + (dy + 1) // 2
        src = (pl.ds(x_lo + t * (nx - deep), deep), slice(None), pl.ds(*src_y), slice(None))
        dst = (pl.ds(x_hi - t * (nx + deep), deep), slice(None), pl.ds(*dst_y), slice(None))
        if send is None:
            return ref.at[dst]
        return pltpu.make_async_remote_copy(
            src_ref=ref.at[src],
            dst_ref=ref.at[dst],
            send_sem=send.at[k],
            recv_sem=recv.at[k],
            device_id={"gx": gx + 2 * t - 1, "gy": gy + dy},
            device_id_type=MESH,
        )

    def start_side(ref, t, dys, width, send, recv):
        for dy in dys:

            @pl.when(has((2 * t - 1, dy)))
            def _():
                side_copy(ref, t, dy, width, send, recv).start()

    def wait_side(ref, t, width, send, recv):
        for dy in (0, -1, 1):
            came = has((1 - 2 * t, -dy))

            @pl.when(came)
            def _():
                side_copy(ref, t, dy, width, send, recv).wait_recv()

            @pl.when(jnp.logical_not(came))
            def _():
                view = side_copy(ref, t, dy, width, None, None)
                view[...] = jnp.zeros(view.shape, F32)

            @pl.when(has((2 * t - 1, dy)))
            def _():
                side_copy(ref, t, dy, width, send, recv).wait_send()

    xs, ys = pl.ds(x_lo, nx), pl.ds(y_lo, ny)

    loads = [
        (res_h, res_s),
        (depth_h, depth_s),
        (csq_h, csq_s),
        (now_h, now_s),
        (prev_h, prev_s),
        (dirn_h, dirn_s),
        (oldg_h, oldg),
    ]
    copies = [
        pltpu.make_async_copy(src, dst, local_sem.at[i]) for i, (src, dst) in enumerate(loads)
    ]
    for copy in copies:
        copy.start()

    half = nx // 2
    gy_core = gys * 2
    place = gy * 2 + core
    partner = {"shot": shot + 1 - 2 * core}
    opposite = {"shot": lax.rem(shot + 2, shots)}

    def gx_member(k):
        return {"gx": k}

    def side_member(k):
        return {"gy": k // 2, "shot": shot - core + lax.rem(k, 2)}

    wide = gy * shots + shot

    def wide_member(k):
        return {"gy": k // shots, "shot": lax.rem(k, shots)}

    barrier = pltpu.get_barrier_semaphore()

    def greet(device):
        pl.semaphore_signal(barrier, inc=1, device_id=device, device_id_type=MESH)

    for o in range(1, gxs):
        greet(gx_member(lax.rem(gx + o, gxs)))
    for o in range(1, gys * shots):
        greet(wide_member(lax.rem(wide + o, gys * shots)))
    met = jnp.int32(gxs + gys * shots - 2)
    for way in WAYS[4:]:

        @pl.when(has(way))
        def _():
            greet({"gx": gx + way[0], "gy": gy + way[1]})

        met = met + has(way).astype(jnp.int32)

    lane = lax.broadcasted_iota(jnp.int32, (ey, LANES), 1)
    row = lax.broadcasted_iota(jnp.int32, (ey, LANES), 0)
    live_here = live[0]

    @pl.loop(0, ex)
    def _(i):
        for h in range(parts):
            adj[0, i, h] = jnp.zeros((ey, LANES), F32)
            hit = (row + (gy * ny - TILE) == source[0, 1]) & (lane + h * LANES == source[0, 2])
            hit = hit & (row * 0 + (i + gx * nx - DEEP) == source[0, 0])
            spot[i, h] = jnp.where(hit, 1.0, 0.0)

    recs[...] = jnp.zeros(recs.shape, F32)

    def unpack_rows(source_ref, target):
        for i in range(nx):
            for h in range(parts):
                target[i + x_lo, h, y_lo:y_hi, :] = source_ref[i, :, h * LANES : (h + 1) * LANES]

    starts = [(traces, DEEP), (csq, DEEP), (back.at[1], DEEP), (back.at[0], 1), (dirn, DEEP)]

    def start_first(i):
        start_halo(starts[i][0], starts[i][1], start_send.at[i], start_recv.at[i])

    copies[0].wait()
    copies[1].wait()
    depths = depth_s[...].astype(F32)
    top = lax.broadcasted_iota(jnp.int32, (8, ny), 0)
    for i in range(nx):
        level = jnp.where(top == 0, depths[i : i + 1], 0.0)
        rest = jnp.zeros((LANES - steps - 8, ny), F32)
        stack = jnp.concatenate([res_s[:, i, :], level, rest], axis=0)
        traces[i + x_lo, 0, y_lo:y_hi, :] = jnp.transpose(stack)
    pl.semaphore_wait(barrier, met)
    start_first(0)
    copies[2].wait()
    unpack_rows(csq_s, csq.at[...])
    start_first(1)
    copies[3].wait()
    unpack_rows(now_s, back.at[1])
    start_first(2)
    copies[4].wait()
    unpack_rows(prev_s, back.at[0])
    start_first(3)
    copies[5].wait()
    unpack_rows(dirn_s, dirn.at[...])
    copies[6].wait()

    wait_halo(traces, DEEP, start_send.at[0], start_recv.at[0])

    def column(i, n, r, count):
        at = lane[:count]
        picked = jnp.where((at == n) & (at < live_here), traces[i, 0, r : r + count, :], 0.0)
        return jnp.sum(picked, axis=1, keepdims=True)

    def receivers(i):
        level = jnp.sum(jnp.where(lane == steps, traces[i, 0], 0.0), axis=1, keepdims=True)
        return [(lane + h * LANES).astype(F32) == level for h in range(parts)]

    @pl.loop(0, ex)
    def _(i):
        for n in range(steps):
            weights[n, i] = jnp.broadcast_to(column(i, n, 0, ey), (ey, LANES))

    wait_halo(csq, DEEP, start_send.at[1], start_recv.at[1])

    @pl.loop(0, ex)
    def _(i):
        for h, here in enumerate(receivers(i)):
            crec[i, h] = jnp.where(here, csq[i, h], 0.0)
            adj[1, i, h] = crec[i, h] * weights[steps - 1, i]
            twice[i, h] = 2.0 - 6.0 * csq[i, h]

    @pl.loop(0, nx)
    def _(i):
        for h, here in enumerate(receivers(i + x_lo)):
            recv_mask[i, h] = jnp.where(here, 1.0, 0.0)[y_lo:y_hi]

    def strip(field, s, i, r, count, extra):
        at = lane[:count]
        first, last = at == 0, at == LANES - 1
        rows = pl.ds(r, count)
        mids = [field[s, i, h, rows, :] for h in range(parts)]
        ups = [pltpu.roll(mid, 1, 1) for mid in mids]
        downs = [pltpu.roll(mid, LANES - 1, 1) for mid in mids]
        for h, mid in enumerate(mids):
            before = ups[h - 1] if h > 0 else 0.0
            after = downs[h + 1] if h < parts - 1 else 0.0
            left = jnp.where(first, before, ups[h])
            right = jnp.where(last, after, downs[h])
            if r > 0:
                above = field[s, i, h, pl.ds(r - 1, count), :]
            else:
                above = pltpu.roll(mid, 1, 0)
            if r + count < ey:
                below = field[s, i, h, pl.ds(r + 1, count), :]
            else:
                below = pltpu.roll(mid, count - 1, 0)
            total = (field[s, i - 1, h, rows, :] + field[s, i + 1, h, rows, :]) + (above + below)
            total = total + (left + right)
            value = csq[i, h, rows, :] * total + twice[i, h, rows, :] * mid
            value = value - field[s - 1, i, h, rows, :] + extra(i, h, r, count)
            field[s + 1, i, h, rows, :] = value

    def plane(field, s, i, whole, extra):
        if whole:
            strip(field, s, i, 0, TILE, extra)
        for r in range(y_lo, y_hi, 16):
            strip(field, s, i, r, 16, extra)
        if whole:
            strip(field, s, i, y_hi, TILE, extra)

    def planes(field, s, lo, hi, whole, extra):
        @pl.loop(lo, hi, unroll=3 if (hi - lo) % 2 else 2)
        def _(i):
            plane(field, s, i, whole, extra)

    def ahead(s):
        amount = wavelet[0, s - 1]
        return lambda i, h, r, count: amount * spot[i, h, r : r + count, :]

    def behind(s):
        n = steps - 1 - s
        return lambda i, h, r, count: crec[i, h, r : r + count, :] * weights[n, i, r : r + count, :]

    def scattered(s):
        return lambda i, h, r, count: (
            gain[i, h, r : r + count, :] * back[s + 1, i, h, r : r + count, :]
        )

    def advance(field, s, make, j, sends, recvs, width):
        first, second = make(s), make(s + 1)
        now, before = lax.rem(j, 2), lax.rem(j + 1, 2)
        send, recv = sends.at[now], recvs.at[now]
        target = field.at[s + 2]
        left, right = x_lo, x_hi - 1

        @pl.when(j > 0)
        def _():
            wait_halo(field.at[s], DEEP, sends.at[before], recvs.at[before], (2, 3))

        for t in (before, now):

            @pl.when(j > 0)
            def _():
                wait_side(field.at[s], 1 - t, DEEP, sends.at[before], recvs.at[before])

            near, inward = left + t * (nx - 1), 1 - 2 * t

            @pl.loop(0, 3, unroll=3)
            def _(i):
                plane(field, s, near - 1 + i, True, first)

            plane(field, s + 1, near, False, second)
            if width == DEEP:
                start_side(target, t, (-1, 1), width, send, recv)
            plane(field, s, near + 2 * inward, True, first)
            plane(field, s + 1, near + inward, False, second)
            start_side(target, t, (0,), width, send, recv)
        planes(field, s, left + 3, right - 2, True, first)
        planes(field, s + 1, left + 2, right - 1, False, second)
        start_way(target, 2, width, send, recv)
        start_way(target, 3, width, send, recv)

    blocks = (steps - 1) // 2
    end = 2 * blocks + 1
    final = (blocks - 1) % 2
    fields = ((adj, 1, behind), (back, 0, ahead))

    def both(j, width):
        s = 2 * j + 1
        for field, way, make in fields:
            if way == 0:

                @pl.when(j == 0)
                def _():
                    wait_halo(back.at[1], DEEP, start_send.at[2], start_recv.at[2])
                    wait_halo(back.at[0], 1, start_send.at[3], start_recv.at[3])

            advance(field, s, make, j, halo_send.at[way], halo_recv.at[way], width)

    @pl.loop(0, blocks - 1)
    def _(j):
        both(j, DEEP)

    both(jnp.int32(blocks - 1), 1)

    def product(i, h, slots):
        terms = [
            back[a, i, h, y_lo:y_hi, :] * adj[steps + 1 - a, i, h, y_lo:y_hi, :] for a in slots
        ]
        return functools.reduce(lambda one, two: one + two, terms)

    @pl.loop(x_lo, x_hi)
    def _(i):
        for h in range(parts):
            grad[i, h, y_lo:y_hi, :] = product(i, h, range(2, steps))

    for field, way, make in fields:
        wait_halo(field.at[end], 1, halo_send.at[way, final], halo_recv.at[way, final])
        planes(field, end, x_lo, x_hi, False, make(end))

    start_first(4)

    mine, other = x_lo + half * core, x_lo + half * (1 - core)

    def complete(i, h):
        return grad[i, h, y_lo:y_hi, :] + product(i, h, (1, steps))

    def pair_copy(src, dst, k, p, device):
        return pltpu.make_async_remote_copy(
            src_ref=src,
            dst_ref=dst,
            send_sem=pair_send.at[k, p],
            recv_sem=pair_recv.at[k, p],
            device_id=device,
            device_id_type=MESH,
        )

    def own_plane(p):
        return grad.at[mine + p, :, ys, :]

    def swap_a(p):
        return pair_copy(half_c.at[p], half_a.at[p], 0, p, partner)

    def swap_b(p):
        return pair_copy(own_plane(p), half_b.at[p], 1, p, opposite)

    def spread(p):
        return pair_copy(own_plane(p), own_plane(p), 2, p, partner)

    def add_plane(p, buffer):
        for h in range(parts):
            grad[mine + p, h, y_lo:y_hi, :] = grad[mine + p, h, y_lo:y_hi, :] + buffer[p, h]

    @pl.loop(0, half)
    def _(p):
        for h in range(parts):
            half_c[p, h] = complete(other + p, h)
        swap_a(p).start()

    @pl.loop(0, half)
    def _(p):
        for h in range(parts):
            grad[mine + p, h, y_lo:y_hi, :] = complete(mine + p, h)
        swap_a(p).wait()
        add_plane(p, half_a)
        swap_b(p).start()

    @pl.loop(0, half)
    def _(p):
        swap_b(p).wait()
        add_plane(p, half_b)
        spread(p).start()

    def fold(values):
        return jnp.sum(values.reshape(-1, 8, LANES), axis=0)

    def dots(i, sums):
        for h in range(parts):
            g = grad[mine + i, h, y_lo:y_hi, :]
            o = oldg[mine + i - x_lo, :, h * LANES : (h + 1) * LANES]
            d = dirn[mine + i, h, y_lo:y_hi, :]
            added = [fold(a * b) for a, b in ((g, g), (g, o), (o, o), (g, d))]
            sums = tuple(s + p for s, p in zip(sums, added))
        return sums

    zero = jnp.zeros((8, LANES), F32)
    eight = lax.broadcasted_iota(jnp.int32, (8, LANES), 0)

    def pack(sums):
        packed = zero
        for k, value in enumerate(sums):
            packed = jnp.where(eight == k, jnp.sum(value, axis=0, keepdims=True), packed)
        return packed

    def unpack(packed, k):
        return jnp.sum(packed[k : k + 1], axis=1, keepdims=True)

    sums = lax.fori_loop(0, half, dots, (zero,) * 4)
    def all_sum(values, slots, at, count, member, base):
        slots[at] = values

        def copy(peer, slot):
            return pltpu.make_async_remote_copy(
                src_ref=slots.at[at],
                dst_ref=slots.at[slot],
                send_sem=sum_send.at[base, peer],
                recv_sem=sum_recv.at[base, slot],
                device_id=member(peer),
                device_id_type=MESH,
            )

        for o in range(1, count):
            copy(lax.rem(at + o, count), at).start()
        for o in range(1, count):
            source_at = lax.rem(at + count - o, count)
            copy(source_at, source_at).wait_recv()
        for o in range(1, count):
            copy(lax.rem(at + o, count), at).wait_send()
        total = slots[0]
        for k in range(1, count):
            total = total + slots[k]
        return total

    stacked = pack(sums)
    for p in range(half):
        spread(p).wait_recv()
    start_halo(grad, DEEP, start_send.at[0], start_recv.at[0])
    stacked = all_sum(stacked, slots_a.at[0], gx, gxs, gx_member, 0)
    stacked = all_sum(stacked, slots_b, place, gy_core, side_member, 1)
    grad_sq, cross, old_sq, toward = [unpack(stacked, k) for k in range(4)]
    beta = (grad_sq - cross) / old_sq
    slope = grad_sq + beta * toward
    for p in range(half):
        spread(p).wait_send()
    wait_halo(dirn, DEEP, start_send.at[4], start_recv.at[4])
    wait_halo(grad, DEEP, start_send.at[0], start_recv.at[0])

    @pl.loop(0, ex)
    def _(i):
        for h in range(parts):
            onward = grad[i, h] + beta * dirn[i, h]
            dirn[i, h] = onward
            gain[i, h] = csq[i, h] * onward
            adj[1, i, h] = gain[i, h] * back[1, i, h]

    def sample(s):
        @pl.loop(0, nx, unroll=2)
        def _(i):
            seen = adj[s, i + x_lo, 0, y_lo:y_hi, :] * recv_mask[i, 0]
            for h in range(1, parts):
                seen = seen + adj[s, i + x_lo, h, y_lo:y_hi, :] * recv_mask[i, h]
            value = jnp.sum(seen, axis=1, keepdims=True)
            recs[i] = jnp.where(lane[:ny] == s - 1, value, recs[i])

    @pl.loop(0, nx)
    def _(i):
        for h in range(parts):
            dirn_s[i, :, h * LANES : (h + 1) * LANES] = grad[i + x_lo, h, y_lo:y_hi, :]

    out_grad = pltpu.make_async_copy(dirn_s, grad_h, out_sem.at[0])
    out_grad.start()
    sample(1)

    def born(j, width):
        s = 2 * j + 1
        advance(adj, s, scattered, j, halo_send.at[2], halo_recv.at[2], width)
        sample(s + 1)
        sample(s + 2)

    @pl.loop(0, blocks - 1)
    def _(j):
        born(j, DEEP)

    born(jnp.int32(blocks - 1), 1)
    wait_halo(adj.at[end], 1, halo_send.at[2, final], halo_recv.at[2, final])
    planes(adj, end, x_lo, x_hi, False, scattered(end))
    sample(end + 1)

    lane_r = lane[:ny]
    told = lane_r < live_here
    kept = lane_r < steps

    def score(i, sums):
        rec = jnp.where(told, recs[i], 0.0)
        res = jnp.where(kept, traces[i + x_lo, 0, y_lo:y_hi, :], 0.0)
        recs[i] = rec
        added = [fold(a * b) for a, b in ((rec, rec), (rec, res), (res, res))]
        return tuple(s + p for s, p in zip(sums, added))

    sums = lax.fori_loop(0, nx, score, (zero,) * 3)
    for i in range(nx):
        resid_s[:, i, :] = jnp.transpose(recs[i])[:steps]

    out_born = pltpu.make_async_copy(resid_s, born_h, out_sem.at[1])
    out_born.start()
    stacked = pack(sums)
    stacked = all_sum(stacked, slots_a.at[1], gx, gxs, gx_member, 2)
    stacked = all_sum(stacked, slots_c, wide, gys * shots, wide_member, 3)
    rec_sq, rec_res, res_sq = [unpack(stacked, k) for k in range(3)]
    length = slope / rec_sq

    misfit = res_sq - 2.0 * length * rec_res + length * length * rec_sq
    scalars = jnp.where(eight == 0, beta, jnp.where(eight == 1, length, misfit * (0.5 / entries)))
    scalars_o[...] = scalars
    out_grad.wait()
    out_born.wait()


def finish(scalars, grad, dirn, refl, residual, born, image, onward, resid, misfit):
    beta, length = scalars[0:1, 0:1], scalars[1:2, 0:1]
    misfit[0, 0] = jnp.sum(scalars[2:3, 0:1])

    @pl.loop(0, grad.shape[0])
    def _(i):
        path = grad[i] + beta * dirn[i]
        onward[i] = path
        image[i] = refl[i] + length * path

    @pl.loop(0, residual.shape[0])
    def _(n):
        resid[n] = residual[n] - length * born[n]


def on_device(groups, *arguments):
    (now, prev, csq, refl, dirn, oldg, residual, depth, source, wavelet, live) = arguments
    now, prev = now[0], prev[0]
    nx, ny, nz = now.shape
    steps = residual.shape[1]
    entries = float(residual.size * groups[0] * groups[1] * groups[2])
    ex, ey = nx + 2 * DEEP, ny + 2 * TILE
    whole = pl.BlockSpec(memory_space=pl.ANY)
    small = pl.BlockSpec(memory_space=pltpu.SMEM)
    parts = nz // LANES
    grow = pltpu.VMEM((ex, parts, ey, LANES), F32)
    block = pltpu.VMEM((nx, parts, ny, LANES), F32)
    stage = pltpu.VMEM((nx, ny, nz), F32)
    piece = pltpu.VMEM((nx // 2, parts, ny, LANES), F32)
    history = pltpu.VMEM((steps + 1, ex, parts, ey, LANES), F32)
    dma = pltpu.SemaphoreType.DMA
    grad, born, scalars = pl.pallas_call(
        functools.partial(kernel, (nx, ny, nz, steps, entries), groups),
        out_shape=(
            jax.ShapeDtypeStruct((nx, ny, nz), F32),
            jax.ShapeDtypeStruct((steps, nx, ny), F32),
            jax.ShapeDtypeStruct((8, 128), F32),
        ),
        in_specs=[whole] * 7 + [small] * 3,
        out_specs=(whole, whole, pl.BlockSpec(memory_space=pltpu.VMEM)),
        scratch_shapes=[
            history,
            history,
            grow,
            grow,
            grow,
            grow,
            grow,
            grow,
            grow,
            pltpu.VMEM((nx, ny, LANES), F32),
            block,
            pltpu.VMEM((ex, 1, ey, LANES), F32),
            pltpu.VMEM((steps, ex, ey, LANES), F32),
            stage,
            stage,
            stage,
            stage,
            stage,
            pltpu.VMEM((steps, nx, ny), F32),
            pltpu.VMEM((nx, ny), jnp.int32),
            pltpu.VMEM((steps, nx, ny), F32),
            piece,
            piece,
            piece,
            pltpu.VMEM((2, groups[1], 8, LANES), F32),
            pltpu.VMEM((groups[2] * 2, 8, LANES), F32),
            pltpu.VMEM((groups[2] * groups[0], 8, LANES), F32),
            dma((7,)),
            dma((5, 8)),
            dma((5, 8)),
            dma((3, 2, 8)),
            dma((3, 2, 8)),
            dma((3, nx // 2)),
            dma((3, nx // 2)),
            dma((4, 16)),
            dma((4, 16)),
            dma((2,)),
        ],
        compiler_params=pltpu.CompilerParams(
            has_side_effects=True, collective_id=0, vmem_limit_bytes=62 * 1024 * 1024
        ),
        name="iteration",
    )(now, prev, csq, dirn, oldg, residual[0], depth[0], source, wavelet, live)
    few = 2
    vector = pl.BlockSpec((8, LANES), lambda i: (0, 0))
    cube = pl.BlockSpec((nx // few, ny, nz), lambda i: (i, 0, 0))
    trace = pl.BlockSpec((steps // few, nx, ny), lambda i: (i, 0, 0))
    image, onward, resid, misfit = pl.pallas_call(
        finish,
        out_shape=(
            jax.ShapeDtypeStruct((nx, ny, nz), F32),
            jax.ShapeDtypeStruct((nx, ny, nz), F32),
            jax.ShapeDtypeStruct((steps, nx, ny), F32),
            jax.ShapeDtypeStruct((1, 1), F32),
        ),
        grid=(few,),
        in_specs=[vector, cube, cube, cube, trace, trace],
        out_specs=(cube, cube, trace, small),
        name="finish",
    )(scalars, grad, dirn, refl, residual[0], born)
    return image, onward, resid[None], misfit[0, 0]


def solution(mesh):
    groups = (mesh.shape["shot"], mesh.shape["gx"], mesh.shape["gy"])
    space = P("gx", "gy", None)
    placed = (
        P("shot", "gx", "gy", None),
        P("shot", "gx", "gy", None),
        space,
        space,
        space,
        space,
        P("shot", None, "gx", "gy"),
        P("shot", "gx", "gy"),
        P("shot", None),
        P("shot", None),
        P("shot"),
    )
    return jax.shard_map(
        functools.partial(on_device, groups),
        mesh=mesh,
        in_specs=placed,
        out_specs=(space, space, P("shot", None, "gx", "gy"), P()),
        check_vma=False,
    )
```
